8 devices in a mesh: inst: 1 (over z), dev: 2 (over y), side: 4 (over x, core).
Axes of the slice: x: 2, y: 2, z: 1, core: 2. Of those that a mesh axis runs over, the one named last changes fastest.
Arguments:
- hidden: bfloat16 [512, 2048], P(('inst', 'dev'))
- k_cache: bfloat16 [1, 512, 16, 128, 128], P(None, ('inst', 'dev'))
- v_cache: bfloat16 [1, 512, 16, 128, 128], P(None, ('inst', 'dev'))
- cache_lens: int32 [512], P(('inst', 'dev'))
- expert_ids: int32 [1, 512, 8], P(None, ('inst', 'dev'))
- route_gates: float32 [1, 512, 8], P(None, ('inst', 'dev'))
- attn_gain: float32 [1, 2048], replicated
- ffn_gain: float32 [1, 2048], replicated
- w_q: bfloat16 [1, 2048, 2048], replicated
- w_kv: bfloat16 [1, 2048, 4096], replicated
- w_o: bfloat16 [1, 2048, 2048], replicated
- shared_gate: bfloat16 [1, 2048, 1024], replicated
- shared_up: bfloat16 [1, 2048, 1024], replicated
- shared_down: bfloat16 [1, 1024, 2048], replicated
- w_gate: bfloat16 [1, 64, 2048, 1024], P(None, 'dev')
- w_up: bfloat16 [1, 64, 2048, 1024], P(None, 'dev')
- w_down: bfloat16 [1, 64, 1024, 2048], P(None, 'dev')
Outputs:
- output: bfloat16 [512, 2048], P(('inst', 'dev'))
All inputs are finite; a program needn't handle non-finite values.
Results may differ from the reference program's by a relative error of at most 0.0163462.
Values are sent between devices in bfloat16 or wider.
A program may use at most 2.75 GiB of HBM per device.

```python
import jax
import jax.numpy as jnp
import math
from jax import lax

MODEL_DIM = 2048
Q_HEADS = 16
KV_HEADS = 16
HEAD_DIM = 128
NUM_EXPERTS = 64
EXPERT_FF = 1024
TOP_K = 8
SHARED_FF = 1024
NUM_LAYERS = 1
CACHE_LEN = 128
BLOCK_TOKENS = 128
NUM_BLOCKS = 4

BATCH = BLOCK_TOKENS * NUM_BLOCKS
EXPERT_CAP = 2 * (BLOCK_TOKENS * TOP_K // NUM_EXPERTS) - 1 + min(1, BLOCK_TOKENS * TOP_K % NUM_EXPERTS)
TOTAL_CAP = NUM_BLOCKS * EXPERT_CAP
NORM_EPS = 1e-6
ROPE_BASE = 10000.0


def draw_routes(route_key):
    total = BLOCK_TOKENS * TOP_K
    base_count = total // NUM_EXPERTS
    spare = total % NUM_EXPERTS
    key_perm, key_shift, key_tok = jax.random.split(route_key, 3)
    expert_order = jax.random.permutation(key_perm, NUM_EXPERTS)
    shifts = jax.random.randint(key_shift, (NUM_EXPERTS // 2,), 0, base_count)
    shifts = shifts.at[0].set(base_count - 1)
    deltas = jnp.stack([shifts, -shifts], axis=1).reshape(NUM_EXPERTS)
    extras = (jnp.arange(NUM_EXPERTS) < spare).astype(jnp.int32)
    counts = jnp.zeros((NUM_EXPERTS,), jnp.int32).at[expert_order].set(base_count + deltas + extras)
    run_ends = jnp.cumsum(counts)
    places = jnp.arange(total)
    expert_of = jnp.sum((run_ends[None, :] <= places[:, None]).astype(jnp.int32), axis=1)
    by_place = expert_of.reshape(TOP_K, BLOCK_TOKENS).T
    tok_order = jax.random.permutation(key_tok, BLOCK_TOKENS)
    return by_place[tok_order]


def setup_inputs(seed: int = 0, part: int = 0) -> dict:
    root_key = jax.random.key(seed)
    part_keys = jax.random.split(jax.random.fold_in(root_key, part), 7)
    shared_keys = jax.random.split(root_key, 11)
    q_width = Q_HEADS * HEAD_DIM
    kv_width = KV_HEADS * HEAD_DIM
    key_scale = (0.5 * math.log(CACHE_LEN)) ** 0.5
    dim_scale = MODEL_DIM ** -0.5
    cache_shape = (NUM_LAYERS, BATCH, KV_HEADS, CACHE_LEN, HEAD_DIM)
    hidden = jax.random.normal(part_keys[0], (BATCH, MODEL_DIM), jnp.float32).astype(jnp.bfloat16)
    k_cache = (key_scale * jax.random.normal(part_keys[1], cache_shape, jnp.float32)).astype(jnp.bfloat16)
    v_mean = jax.random.normal(part_keys[2], (NUM_LAYERS, BATCH, KV_HEADS, 1, HEAD_DIM), jnp.float32)
    v_cache = (0.6 * v_mean + 0.8 * jax.random.normal(part_keys[3], cache_shape, jnp.float32)).astype(jnp.bfloat16)
    cache_lens = jax.random.randint(part_keys[4], (BATCH,), CACHE_LEN // 4, CACHE_LEN + 1)
    cache_lens = cache_lens.at[0].set(CACHE_LEN).at[1].set(CACHE_LEN // 4)
    route_keys = jax.random.split(part_keys[5], NUM_LAYERS * NUM_BLOCKS)
    expert_ids = jax.vmap(draw_routes)(route_keys).reshape(NUM_LAYERS, BATCH, TOP_K)
    route_gates = jax.random.uniform(part_keys[6], (NUM_LAYERS, BATCH, TOP_K), jnp.float32, 0.3, 1.0)
    attn_gain = jax.random.uniform(shared_keys[0], (NUM_LAYERS, MODEL_DIM), jnp.float32, 0.5, 1.5)
    ffn_gain = jax.random.uniform(shared_keys[1], (NUM_LAYERS, MODEL_DIM), jnp.float32, 0.5, 1.5)
    w_q = (dim_scale * jax.random.normal(shared_keys[2], (NUM_LAYERS, MODEL_DIM, q_width), jnp.float32)).astype(jnp.bfloat16)
    kv_cols = jnp.array([key_scale, CACHE_LEN / 8.0], jnp.float32)[None, None, :, None] * dim_scale
    w_kv = (kv_cols * jax.random.normal(shared_keys[3], (NUM_LAYERS, MODEL_DIM, 2, kv_width), jnp.float32)).reshape(NUM_LAYERS, MODEL_DIM, 2 * kv_width).astype(jnp.bfloat16)
    w_o = (q_width ** -0.5 * jax.random.normal(shared_keys[4], (NUM_LAYERS, q_width, MODEL_DIM), jnp.float32)).astype(jnp.bfloat16)
    shared_gate = (dim_scale * jax.random.normal(shared_keys[5], (NUM_LAYERS, MODEL_DIM, SHARED_FF), jnp.float32)).astype(jnp.bfloat16)
    shared_up = (dim_scale * jax.random.normal(shared_keys[6], (NUM_LAYERS, MODEL_DIM, SHARED_FF), jnp.float32)).astype(jnp.bfloat16)
    shared_down = (SHARED_FF ** -0.5 * jax.random.normal(shared_keys[7], (NUM_LAYERS, SHARED_FF, MODEL_DIM), jnp.float32)).astype(jnp.bfloat16)
    w_gate = (dim_scale * jax.random.normal(shared_keys[8], (NUM_LAYERS, NUM_EXPERTS, MODEL_DIM, EXPERT_FF), jnp.float32)).astype(jnp.bfloat16)
    w_up = (dim_scale * jax.random.normal(shared_keys[9], (NUM_LAYERS, NUM_EXPERTS, MODEL_DIM, EXPERT_FF), jnp.float32)).astype(jnp.bfloat16)
    w_down = (EXPERT_FF ** -0.5 * jax.random.normal(shared_keys[10], (NUM_LAYERS, NUM_EXPERTS, EXPERT_FF, MODEL_DIM), jnp.float32)).astype(jnp.bfloat16)
    return {'hidden': hidden, 'k_cache': k_cache, 'v_cache': v_cache, 'cache_lens': cache_lens, 'expert_ids': expert_ids, 'route_gates': route_gates, 'attn_gain': attn_gain, 'ffn_gain': ffn_gain, 'w_q': w_q, 'w_kv': w_kv, 'w_o': w_o, 'shared_gate': shared_gate, 'shared_up': shared_up, 'shared_down': shared_down, 'w_gate': w_gate, 'w_up': w_up, 'w_down': w_down}


def rms_norm(in_rows, norm_gain):
    rows_f = in_rows.astype(jnp.float32)
    inv_rms = lax.rsqrt(jnp.mean(rows_f * rows_f, axis=-1, keepdims=True) + NORM_EPS)
    return (rows_f * inv_rms * norm_gain).astype(jnp.bfloat16)


def rotate_pos(in_vecs, positions):
    half_dim = in_vecs.shape[-1] // 2
    inv_freq = ROPE_BASE ** (-jnp.arange(half_dim, dtype=jnp.float32) * 2.0 / in_vecs.shape[-1])
    angles = positions.astype(jnp.float32)[:, None] * inv_freq[None, :]
    cosine = jnp.cos(angles)[:, None, :]
    sine_part = jnp.sin(angles)[:, None, :]
    first_half = in_vecs[..., :half_dim]
    second = in_vecs[..., half_dim:]
    return jnp.concatenate([first_half * cosine - second * sine_part, second * cosine + first_half * sine_part], axis=-1)


def swiglu(in_rows, gate_w, up_w, down_w):
    act_gate = jnp.dot(in_rows, gate_w, preferred_element_type=jnp.float32)
    act_up = jnp.dot(in_rows, up_w, preferred_element_type=jnp.float32)
    inner_act = (jax.nn.silu(act_gate) * act_up).astype(jnp.bfloat16)
    return jnp.dot(inner_act, down_w, preferred_element_type=jnp.float32).astype(jnp.bfloat16)


def attend_block(blk_pack, wq_l, wkv_l, wo_l):
    in_rows, key_blk, val_blk, lens_blk = blk_pack
    tokens = in_rows.shape[0]
    groups = Q_HEADS // KV_HEADS
    q_rows = jnp.dot(in_rows, wq_l, preferred_element_type=jnp.float32).astype(jnp.bfloat16)
    fresh_kv = jnp.dot(in_rows, wkv_l, preferred_element_type=jnp.float32).astype(jnp.bfloat16).reshape(tokens, 2, KV_HEADS, HEAD_DIM)
    q_rows = rotate_pos(q_rows.astype(jnp.float32).reshape(tokens, Q_HEADS, HEAD_DIM), lens_blk).astype(jnp.bfloat16).reshape(tokens, KV_HEADS, groups, HEAD_DIM)
    new_key = rotate_pos(fresh_kv[:, 0].astype(jnp.float32), lens_blk).astype(jnp.bfloat16)
    new_val = fresh_kv[:, 1]
    score_scale = HEAD_DIM ** -0.5
    scores = jnp.einsum('tkgd,tksd->tkgs', q_rows.astype(jnp.float32), key_blk.astype(jnp.float32)) * score_scale
    valid_mask = jnp.arange(CACHE_LEN)[None, None, None, :] < lens_blk[:, None, None, None]
    scores = jnp.where(valid_mask, scores, -jnp.inf)
    self_score = jnp.einsum('tkgd,tkd->tkg', q_rows.astype(jnp.float32), new_key.astype(jnp.float32)) * score_scale
    peak_score = jnp.maximum(jnp.max(scores, axis=-1), self_score)
    weights = jnp.exp(scores - peak_score[..., None])
    self_weight = jnp.exp(self_score - peak_score)
    denom_sum = jnp.sum(weights, axis=-1) + self_weight
    prob_bf = (weights / denom_sum[..., None]).astype(jnp.bfloat16)
    self_prob = (self_weight / denom_sum).astype(jnp.bfloat16)
    context = jnp.einsum('tkgs,tksd->tkgd', prob_bf.astype(jnp.float32), val_blk.astype(jnp.float32))
    context = context + self_prob.astype(jnp.float32)[..., None] * new_val.astype(jnp.float32)[:, :, None, :]
    context = context.astype(jnp.bfloat16).reshape(tokens, Q_HEADS * HEAD_DIM)
    return jnp.dot(context, wo_l, preferred_element_type=jnp.float32)


def reference(hidden, k_cache, v_cache, cache_lens, expert_ids, route_gates, attn_gain, ffn_gain, w_q, w_kv, w_o, shared_gate, shared_up, shared_down, w_gate, w_up, w_down):
    lens_blocks = cache_lens.reshape(NUM_BLOCKS, BLOCK_TOKENS)
    expert_range = jnp.arange(NUM_EXPERTS)
    owner_idx = jnp.arange(BATCH * TOP_K) // TOP_K

    def layer_step(x_state, layer_pack):
        keys_l, vals_l, ids_l, gates_l, gain_a, gain_f, wq_l, wkv_l, wo_l, sg_l, su_l, sd_l, eg_l, eu_l, ed_l = layer_pack
        normed = rms_norm(x_state, gain_a)
        block_pack = (normed.reshape(NUM_BLOCKS, BLOCK_TOKENS, MODEL_DIM), keys_l.reshape(NUM_BLOCKS, BLOCK_TOKENS, KV_HEADS, CACHE_LEN, HEAD_DIM), vals_l.reshape(NUM_BLOCKS, BLOCK_TOKENS, KV_HEADS, CACHE_LEN, HEAD_DIM), lens_blocks)
        attn_out = lax.map(lambda blk_pack: attend_block(blk_pack, wq_l, wkv_l, wo_l), block_pack).reshape(BATCH, MODEL_DIM)
        mid_rows = (x_state.astype(jnp.float32) + attn_out).astype(jnp.bfloat16)
        ffn_in = rms_norm(mid_rows, gain_f)
        shared_out = swiglu(ffn_in, sg_l, su_l, sd_l)
        flat_ids = ids_l.reshape(BATCH * TOP_K)
        onehot = (flat_ids[:, None] == expert_range[None, :]).astype(jnp.int32)
        slot_ids = jnp.sum((jnp.cumsum(onehot, axis=0) - onehot) * onehot, axis=1)
        slot_table = jnp.zeros((NUM_EXPERTS, TOTAL_CAP), jnp.int32).at[flat_ids, slot_ids].set(owner_idx)
        expert_rows = ffn_in[slot_table]
        expert_out = lax.map(lambda expert_pack: swiglu(expert_pack[0], expert_pack[1], expert_pack[2], expert_pack[3]), (expert_rows, eg_l, eu_l, ed_l))
        picked = expert_out[flat_ids, slot_ids].reshape(BATCH, TOP_K, MODEL_DIM)
        routed = jnp.sum(gates_l[:, :, None] * picked.astype(jnp.float32), axis=1)
        new_state = (mid_rows.astype(jnp.float32) + shared_out.astype(jnp.float32) + routed).astype(jnp.bfloat16)
        return new_state, None

    layer_stack = (k_cache, v_cache, expert_ids, route_gates, attn_gain, ffn_gain, w_q, w_kv, w_o, shared_gate, shared_up, shared_down, w_gate, w_up, w_down)
    return lax.scan(layer_step, hidden, layer_stack)[0]
```

```python
import functools

import numpy as np
import jax
import jax.numpy as jnp
from jax import lax
from jax.experimental import pallas as pl
from jax.experimental.pallas import tpu as pltpu
from jax.sharding import PartitionSpec as P

NORM_EPS = 1e-6
ROPE_BASE = 10000.0
MESH = pl.DeviceIdType.MESH
F32 = jnp.float32
BF16 = jnp.bfloat16

ROWS = 128
HEADS = 8
HD = 128
DIM = 2048
HALF = DIM // 2
GROUP = 8
KV_RING = 4
RING = 16
EXPERTS = 16
SLOTS = 32
CHUNKS = 4
CW = HALF // CHUNKS
FIRST_AXIS = (1, 0, 1, 1)


def norm_rows(rows_f, gain):
    inv_rms = lax.rsqrt(jnp.mean(rows_f * rows_f, axis=-1, keepdims=True) + NORM_EPS)
    return (rows_f * inv_rms * gain).astype(BF16)


def attn_kernel(lens_ref, hidden_ref, gain_ref, freq_ref, wq_ref, wkv_ref, kc_ref, vc_ref, ctx_ref,
                xbuf, wbuf, pos_buf, q3, k3, v3, c3, sbuf, kbuf, vbuf, xsem, wsem, ksem, vsem):
    side = lax.axis_index('side')
    row0 = (side // 2) * ROWS
    core = side % 2
    h0 = core * HEADS
    groups = ROWS // GROUP

    def kv_copies(tok, slot):
        size = pl.multiple_of(((lens_ref[row0 + tok] + 15) // 16) * 16, 16)
        k_cp = pltpu.make_async_copy(kc_ref.at[0, row0 + tok, pl.ds(h0, HEADS), pl.ds(0, size), :],
                                     kbuf.at[slot, :, pl.ds(0, size), :], ksem.at[slot])
        v_cp = pltpu.make_async_copy(vc_ref.at[0, row0 + tok, pl.ds(h0, HEADS), pl.ds(0, size), :],
                                     vbuf.at[slot, :, pl.ds(0, size), :], vsem.at[slot])
        return k_cp, v_cp

    def start_group(grp):
        for i in range(GROUP):
            k_cp, v_cp = kv_copies(grp * GROUP + i, lax.rem(grp, KV_RING) * GROUP + i)
            k_cp.start()
            v_cp.start()

    x_cp = pltpu.make_async_copy(hidden_ref.at[pl.ds(row0, ROWS), :], xbuf, xsem)
    x_cp.start()
    w_cps = []
    for i in range(6):
        kind, j = i // 2, i % 2
        col = core * HALF + j * 512
        if kind == 0:
            src = wq_ref.at[0, :, pl.ds(col, 512)]
        else:
            src = wkv_ref.at[0, :, pl.ds((kind - 1) * DIM + col, 512)]
        cp = pltpu.make_async_copy(src, wbuf.at[i], wsem.at[i])
        cp.start()
        w_cps.append(cp)

    def zero_slot(i, carry):
        vbuf[i] = jnp.zeros((HEADS, HD, HD), BF16)
        return carry
    lax.fori_loop(0, KV_RING * GROUP, zero_slot, 0)

    start_group(jnp.int32(0))
    start_group(jnp.int32(1))

    def fill_pos(i, carry):
        pos_buf[pl.ds(i, 1), :] = jnp.full((1, HD), lens_ref[row0 + i].astype(F32), F32)
        return carry
    lax.fori_loop(0, ROWS, fill_pos, 0)
    angles = pos_buf[...] * freq_ref[...]
    cosine = jnp.cos(angles)
    lane = lax.broadcasted_iota(jnp.int32, (ROWS, HD), 1)
    sine = jnp.where(lane < HD // 2, -jnp.sin(angles), jnp.sin(angles))

    x_cp.wait()
    normed = norm_rows(xbuf[...].astype(F32), gain_ref[...])
    for i in range(6):
        kind, j = i // 2, i % 2
        w_cps[i].wait()
        res = jnp.dot(normed, wbuf[i], preferred_element_type=F32).astype(BF16).astype(F32)
        for hh in range(4):
            h = j * 4 + hh
            val = res[:, hh * HD:(hh + 1) * HD]
            if kind < 2:
                val = (val * cosine + pltpu.roll(val, HD // 2, 1) * sine).astype(BF16).astype(F32)
            (q3, k3, v3)[kind][:, h, :] = val
        if i == 1:
            start_group(jnp.int32(2))
        if i == 3:
            start_group(jnp.int32(3))

    row_id = lax.broadcasted_iota(jnp.int32, (HEADS, HD), 0)
    lane_id = lax.broadcasted_iota(jnp.int32, (HEADS, HD), 1)

    def wait_kv(grp, which):
        for i in range(GROUP):
            kv_copies(grp * GROUP + i, lax.rem(grp, KV_RING) * GROUP + i)[which].wait()

    def score_group(grp):
        for i in range(GROUP):
            tok = grp * GROUP + i
            slot = lax.rem(grp, KV_RING) * GROUP + i
            keys = kbuf[slot].reshape(HEADS * HD, HD)
            full = lax.dot_general(q3[tok].astype(BF16), keys, (((1,), (1,)), ((), ())), preferred_element_type=F32)
            sc = jnp.zeros((HEADS, HD), F32)
            for h in range(HEADS):
                sc = jnp.where(row_id == h, full[:, h * HD:(h + 1) * HD], sc)
            sbuf[lax.rem(grp, 2), i] = jnp.where(lane_id < lens_ref[row0 + tok], sc * (HD ** -0.5), -jnp.inf)

    def value_group(grp):
        for i in range(GROUP):
            tok = grp * GROUP + i
            slot = lax.rem(grp, KV_RING) * GROUP + i
            sc = sbuf[lax.rem(grp, 2), i]
            self_sc = jnp.sum(q3[tok] * k3[tok], axis=-1, keepdims=True) * (HD ** -0.5)
            peak = jnp.maximum(jnp.max(sc, axis=-1, keepdims=True), self_sc)
            wts = jnp.exp(sc - peak)
            self_w = jnp.exp(self_sc - peak)
            denom = jnp.sum(wts, axis=-1, keepdims=True) + self_w
            prob = wts / denom
            self_p = (self_w / denom).astype(BF16).astype(F32)
            wide = jnp.concatenate([jnp.where(row_id == h, prob, 0.0) for h in range(HEADS)], axis=1).astype(BF16)
            vals = vbuf[slot].reshape(HEADS * HD, HD)
            ctx = jnp.dot(wide, vals, preferred_element_type=F32)
            c3[tok] = ctx + self_p * v3[tok]

    wait_kv(jnp.int32(0), 0)
    score_group(jnp.int32(0))

    def body(grp, carry):
        wait_kv(grp, 1)
        wait_kv(grp + 1, 0)
        value_group(grp)
        score_group(grp + 1)

        @pl.when(grp + KV_RING < groups)
        def _():
            for i in range(GROUP):
                nxt = grp + KV_RING
                for cp in kv_copies(nxt * GROUP + i, lax.rem(nxt, KV_RING) * GROUP + i):
                    cp.start()
        return carry
    lax.fori_loop(0, groups - 1, body, 0)
    wait_kv(jnp.int32(groups - 1), 1)
    value_group(jnp.int32(groups - 1))
    for h in range(HEADS):
        ctx_ref[:, h * HD:(h + 1) * HD] = c3[:, h, :].astype(BF16)


def attention(hidden, lens, gain, w_q, w_kv, k_cache, v_cache):
    freq = ROPE_BASE ** (-np.arange(HD // 2, dtype=np.float64) * 2.0 / HD)
    freq = np.concatenate([freq, freq])[None, :].astype(np.float32)
    any_spec = pl.BlockSpec(memory_space=pl.ANY)
    vmem_spec = pl.BlockSpec(memory_space=pltpu.VMEM)
    slots = KV_RING * GROUP
    return pl.pallas_call(
        attn_kernel,
        out_shape=jax.ShapeDtypeStruct((ROWS, HALF), BF16),
        in_specs=[pl.BlockSpec(memory_space=pltpu.SMEM), any_spec, vmem_spec, vmem_spec] + [any_spec] * 4,
        out_specs=vmem_spec,
        scratch_shapes=[
            pltpu.VMEM((ROWS, DIM), BF16),
            pltpu.VMEM((6, DIM, 512), BF16),
            pltpu.VMEM((ROWS, HD), F32),
            pltpu.VMEM((ROWS, HEADS, HD), F32),
            pltpu.VMEM((ROWS, HEADS, HD), F32),
            pltpu.VMEM((ROWS, HEADS, HD), F32),
            pltpu.VMEM((ROWS, HEADS, HD), F32),
            pltpu.VMEM((2, GROUP, HEADS, HD), F32),
            pltpu.VMEM((slots, HEADS, HD, HD), BF16),
            pltpu.VMEM((slots, HEADS, HD, HD), BF16),
            pltpu.SemaphoreType.DMA,
            pltpu.SemaphoreType.DMA((6,)),
            pltpu.SemaphoreType.DMA((slots,)),
            pltpu.SemaphoreType.DMA((slots,)),
        ],
        compiler_params=pltpu.CompilerParams(vmem_limit_bytes=60 * 1024 * 1024),
        name='attend',
    )(lens, hidden, gain, jnp.asarray(freq), w_q, w_kv, k_cache, v_cache)


def moe_kernel(ctx_ref, rt_ref, gain_ref, hidden_ref, wo_ref, sg_ref, su_ref, sd_ref, wg_ref, wu_ref, wd_ref, out_ref,
               ring, ctx_sib, xbuf, mbuf, uall, ish, base, rt_all, dmat, cg, xe, inner, ybuf, pbuf, recv1, send2, recv2, oall,
               ring_sem, x_sem, misc_s, misc_r, u_s, u_r, uf_s, uf_r, in_s, in_r, p1_s, p1_r, p2_s, p2_r,
               os_s, os_r, ox_s, ox_r, of_s, of_r, out_sem):
    inst = lax.axis_index('inst')
    dy = lax.axis_index('dev')
    side = lax.axis_index('side')
    cx = side // 2
    core = side % 2
    blk0 = dy * 2 + cx
    col0 = core * HALF

    def dev_of(y, x, c):
        return (inst, y, x * 2 + c)
    sibling = dev_of(dy, cx, 1 - core)
    x_nbr = dev_of(dy, 1 - cx, core)
    y_nbr = dev_of(1 - dy, cx, core)
    diag = dev_of(1 - dy, 1 - cx, core)

    def rdma(src, dst, s_sem, r_sem, dev):
        return pltpu.make_async_remote_copy(src_ref=src, dst_ref=dst, send_sem=s_sem, recv_sem=r_sem,
                                            device_id=dev, device_id_type=MESH)

    def start_wo(j):
        pltpu.make_async_copy(wo_ref.at[0, :, pl.ds(col0 + j * 512, 512)], ring.at[j], ring_sem.at[j]).start()

    def start_gate(e, slot):
        pltpu.make_async_copy(wg_ref.at[0, cx * EXPERTS + e, :, pl.ds(core * 512, 512)], ring.at[slot], ring_sem.at[slot]).start()

    def start_up(e, slot):
        pltpu.make_async_copy(wu_ref.at[0, cx * EXPERTS + e, :, pl.ds(core * 512, 512)], ring.at[slot], ring_sem.at[slot]).start()

    def start_down(m, slot):
        k = m // 4
        g = m % 4
        for i in range(4):
            pltpu.make_async_copy(wd_ref.at[0, cx * EXPERTS + g * 4 + i, :, pl.ds(col0 + k * CW, CW)],
                                  ring.at[slot, pl.ds((i // 2) * 1024, 1024), pl.ds((i % 2) * CW, CW)],
                                  ring_sem.at[slot]).start()

    def wait_slot(slot):
        pltpu.make_async_copy(wg_ref.at[0, 0, :, pl.ds(0, 512)], ring.at[slot], ring_sem.at[slot]).wait()

    def start_gu_block(b):
        e, up = (b - 5) // 2, (b - 5) % 2
        (start_up if up else start_gate)(e, b % RING)

    x_cp = pltpu.make_async_copy(hidden_ref.at[pl.ds(cx * ROWS, ROWS), pl.ds(col0, HALF)], xbuf, x_sem)
    x_cp.start()
    start_wo(0)
    start_wo(1)
    pltpu.make_async_copy(sg_ref.at[0, :, pl.ds(core * 512, 512)], ring.at[2], ring_sem.at[2]).start()
    pltpu.make_async_copy(su_ref.at[0, :, pl.ds(core * 512, 512)], ring.at[3], ring_sem.at[3]).start()
    for j in range(2):
        pltpu.make_async_copy(sd_ref.at[0, :, pl.ds(col0 + j * 512, 512)], ring.at[4, pl.ds(j * 1024, 1024), :],
                              ring_sem.at[4]).start()
    for b in range(5, RING):
        start_gu_block(b)

    barrier = pltpu.get_barrier_semaphore()
    for dev in (sibling, x_nbr, y_nbr, diag):
        pl.semaphore_signal(barrier, inc=1, device_id=dev, device_id_type=MESH)
    pl.semaphore_wait(barrier, 4)

    ctx_cp = rdma(ctx_ref, ctx_sib, misc_s.at[0], misc_r.at[0], sibling)
    ctx_cp.start()
    rt_cp = rdma(rt_ref, rt_all.at[dy], misc_s.at[1], misc_r.at[1], y_nbr)
    rt_cp.start()
    rt_all[dy] = rt_ref[...]

    wait_slot(0)
    wait_slot(1)
    x_cp.wait()
    own_row = core * HALF
    sib_row = (1 - core) * HALF
    accs = [jnp.dot(ctx_ref[...], ring[j, pl.ds(own_row, HALF), :], preferred_element_type=F32) for j in range(2)]
    ctx_cp.wait_recv()
    for j in range(2):
        acc = accs[j] + jnp.dot(ctx_sib[...], ring[j, pl.ds(sib_row, HALF), :], preferred_element_type=F32)
        mbuf[core, :, j * 512:(j + 1) * 512] = (xbuf[:, j * 512:(j + 1) * 512].astype(F32) + acc).astype(BF16)
    start_gu_block(16)
    start_gu_block(17)
    m_cp = rdma(mbuf.at[core], mbuf.at[core], misc_s.at[2], misc_r.at[2], sibling)
    m_cp.start()
    rdma(mbuf.at[1 - core], mbuf.at[1 - core], misc_s.at[2], misc_r.at[2], sibling).wait_recv()
    m_lo = mbuf[0].astype(F32)
    m_hi = mbuf[1].astype(F32)
    total = jnp.sum(m_lo * m_lo, axis=-1, keepdims=True) + jnp.sum(m_hi * m_hi, axis=-1, keepdims=True)
    inv_rms = lax.rsqrt(total / DIM + NORM_EPS)
    uall[blk0, :, 0:HALF] = (m_lo * inv_rms * gain_ref[:, 0:HALF]).astype(BF16)
    uall[blk0, :, HALF:DIM] = (m_hi * inv_rms * gain_ref[:, HALF:DIM]).astype(BF16)

    def u_part(b, c):
        return uall.at[b, pl.ds(c * 64, 64), :]
    u_cps = [rdma(u_part(blk0, core), u_part(blk0, core), u_s.at[r], u_r.at[r], dev)
             for r, dev in enumerate((x_nbr, y_nbr, diag))]
    for r in (2, 1, 0):
        u_cps[r].start()

    wait_slot(2)
    wait_slot(3)
    u_own = uall[blk0]
    gate = jnp.dot(u_own, ring[2], preferred_element_type=F32)
    up = jnp.dot(u_own, ring[3], preferred_element_type=F32)
    ish[core] = (jax.nn.silu(gate) * up).astype(BF16)
    start_gu_block(18)
    start_gu_block(19)
    ish_cp = rdma(ish.at[core], ish.at[core], misc_s.at[3], misc_r.at[3], sibling)
    ish_cp.start()

    rt_cp.wait_send()
    rdma(rt_all.at[1 - dy], rt_all.at[1 - dy], misc_s.at[1], misc_r.at[1], y_nbr).wait_recv()
    expert_id = (dy * 32 + cx * EXPERTS + lax.broadcasted_iota(jnp.int32, (EXPERTS, ROWS), 0)).astype(F32)
    before = (lax.broadcasted_iota(jnp.int32, (ROWS, ROWS), 0) < lax.broadcasted_iota(jnp.int32, (ROWS, ROWS), 1))
    before = jnp.where(before, 1.0, 0.0).astype(BF16)
    slot_id = lax.broadcasted_iota(jnp.int32, (SLOTS, ROWS), 0).astype(F32)
    for yb in range(2):
        for xb in range(2):
            b = yb * 2 + xb
            hit = jnp.zeros((EXPERTS, ROWS), F32)
            wts = jnp.zeros((EXPERTS, ROWS), F32)
            for j in range(8):
                same = rt_all[yb, j:j + 1, xb * ROWS:(xb + 1) * ROWS] == expert_id
                hit = jnp.where(same, 1.0, hit)
                wts = jnp.where(same, rt_all[yb, 8 + j:9 + j, xb * ROWS:(xb + 1) * ROWS], wts)
            place = jnp.dot(hit.astype(BF16), before, preferred_element_type=F32)
            place = jnp.where(hit > 0.5, place, -1.0)
            pieces = []
            for e in range(EXPERTS):
                match = place[e:e + 1, :] == slot_id
                dmat[b, e * SLOTS:(e + 1) * SLOTS, :] = jnp.where(match, 1.0, 0.0).astype(BF16)
                pieces.append(jnp.where(match, wts[e:e + 1, :], 0.0))
            for q in range(4):
                part = jnp.concatenate(pieces[q * 4:(q + 1) * 4], axis=0).T
                high = part.astype(BF16)
                rest = part - high.astype(F32)
                mid = rest.astype(BF16)
                low = (rest - mid.astype(F32)).astype(BF16)
                cg[b, 0:128, q * 128:(q + 1) * 128] = high
                cg[b, 128:256, q * 128:(q + 1) * 128] = mid
                cg[b, 256:384, q * 128:(q + 1) * 128] = low

    def dispatch(b):
        def one(n, carry):
            cols = pl.ds(pl.multiple_of(n * 512, 512), 512)
            rows = jnp.dot(dmat[b], uall[b, :, cols], preferred_element_type=F32).astype(BF16)
            for e in range(EXPERTS):
                xe[e, pl.ds(pl.multiple_of(b * SLOTS, SLOTS), SLOTS), cols] = rows[e * SLOTS:(e + 1) * SLOTS, :]
            return carry
        lax.fori_loop(0, DIM // 512, one, 0)

    dispatch(blk0)
    rdma(ish.at[1 - core], ish.at[1 - core], misc_s.at[3], misc_r.at[3], sibling).wait_recv()
    wait_slot(4)
    for j in range(2):
        acc = jnp.dot(ish[0], ring[4, j * 1024:j * 1024 + 512, :], preferred_element_type=F32)
        acc = acc + jnp.dot(ish[1], ring[4, j * 1024 + 512:(j + 1) * 1024, :], preferred_element_type=F32)
        base[:, j * 512:(j + 1) * 512] = mbuf[core, :, j * 512:(j + 1) * 512].astype(F32) + acc.astype(BF16).astype(F32)
    start_gu_block(20)

    blk_of = (dy * 2 + 1 - cx, (1 - dy) * 2 + cx, (1 - dy) * 2 + 1 - cx)
    fwd = []
    for r in (1, 0, 2):
        b = blk_of[r]
        rdma(u_part(b, core), u_part(b, core), u_s.at[r], u_r.at[r], sibling).wait_recv()
        cp = rdma(u_part(b, core), u_part(b, core), uf_s.at[r], uf_r.at[r], sibling)
        cp.start()
        fwd.append(cp)
        rdma(u_part(b, 1 - core), u_part(b, 1 - core), uf_s.at[r], uf_r.at[r], sibling).wait_recv()
        dispatch(b)

    def in_part(e, c):
        return inner.at[e, :, pl.ds(pl.multiple_of(c * 512, 512), 512)]

    def expert_up(e):
        slot_g = lax.rem(5 + 2 * e, RING)
        slot_u = lax.rem(6 + 2 * e, RING)
        wait_slot(slot_g)
        wait_slot(slot_u)
        rows = xe[e]
        gate = jnp.dot(rows, ring[slot_g], preferred_element_type=F32)
        up = jnp.dot(rows, ring[slot_u], preferred_element_type=F32)
        inner[e, :, pl.ds(pl.multiple_of(core * 512, 512), 512)] = (jax.nn.silu(gate) * up).astype(BF16)
        rdma(in_part(e, core), in_part(e, core), in_s.at[e], in_r.at[e], sibling).start()
        return slot_g, slot_u

    def first_half(e, carry):
        slot_g, slot_u = expert_up(e)
        start_gate(e + 8, slot_g)
        start_up(e + 8, slot_u)
        return carry
    lax.fori_loop(0, 8, first_half, 0)

    def second_half(e, carry):
        slot_g, slot_u = expert_up(e)
        start_down(2 * (e - 8), slot_g)
        start_down(2 * (e - 8) + 1, slot_u)
        return carry
    lax.fori_loop(8, 16, second_half, 0)

    def block_at(y, x):
        return y * 2 + x

    def stage1(k):
        axis = FIRST_AXIS[k]
        if axis == 1:
            far, near = block_at(1 - dy, 1 - cx), block_at(1 - dy, cx)
            dev = y_nbr
        else:
            far, near = block_at(1 - dy, 1 - cx), block_at(dy, 1 - cx)
            dev = x_nbr
        return [rdma(pbuf.at[k, b], recv1.at[k, i], p1_s.at[k, i], p1_r.at[k, i], dev) for i, b in enumerate((far, near))]

    def stage2(k):
        axis = FIRST_AXIS[k]
        dev = x_nbr if axis == 1 else y_nbr
        return rdma(send2.at[k], recv2.at[k], p2_s.at[k], p2_r.at[k], dev)

    def run_stage2(k):
        axis = FIRST_AXIS[k]
        b = block_at(dy, 1 - cx) if axis == 1 else block_at(1 - dy, cx)
        stage1(k)[0].wait_recv()
        send2[k] = pbuf[k, b] + recv1[k, 0]
        stage2(k).start()

    def o_part(x, c, k):
        return oall.at[x, c, k]

    def run_final(k):
        stage1(k)[1].wait_recv()
        stage2(k).wait_recv()
        routed = pbuf[k, blk0] + recv1[k, 1] + recv2[k]
        oall[cx, core, k] = (base[:, k * CW:(k + 1) * CW] + routed).astype(BF16)
        mine = o_part(cx, core, k)
        rdma(mine, mine, os_s.at[k], os_r.at[k], sibling).start()
        rdma(mine, mine, ox_s.at[k], ox_r.at[k], x_nbr).start()
        store_out(cx, core, k, 0).start()

    def store_out(x, c, k, which):
        return pltpu.make_async_copy(o_part(x, c, k),
                                     out_ref.at[pl.ds(x * ROWS, ROWS), pl.ds(pl.multiple_of(c * HALF + k * CW, CW), CW)],
                                     out_sem.at[which, k])

    def run_forward(k):
        theirs = o_part(1 - cx, core, k)
        rdma(theirs, theirs, ox_s.at[k], ox_r.at[k], x_nbr).wait_recv()
        rdma(theirs, theirs, of_s.at[k], of_r.at[k], sibling).start()
        store_out(1 - cx, core, k, 1).start()

    for e in range(EXPERTS):
        rdma(in_part(e, 1 - core), in_part(e, 1 - core), in_s.at[e], in_r.at[e], sibling).wait_recv()

    for k in range(CHUNKS):
        def down_group(g, carry):
            slot = lax.rem(5 + 4 * k + g, RING)
            wait_slot(slot)
            for i in range(4):
                e = g * 4 + i
                w = ring[slot, (i // 2) * 1024:(i // 2 + 1) * 1024, (i % 2) * CW:(i % 2 + 1) * CW]
                res = jnp.dot(inner[e], w, preferred_element_type=F32).astype(BF16)
                for b in range(4):
                    ybuf[b, pl.ds(pl.multiple_of(e * SLOTS, SLOTS), SLOTS), :] = res[b * SLOTS:(b + 1) * SLOTS, :]
            return carry
        lax.fori_loop(0, 4, down_group, 0)

        def combine(b, carry):
            res = jnp.dot(cg[b], ybuf[b], preferred_element_type=F32)
            pbuf[k, b] = res[0:128] + res[128:256] + res[256:384]
            return carry
        lax.fori_loop(0, 4, combine, 0)
        for cp in stage1(k):
            cp.start()
        if k >= 1:
            run_stage2(k - 1)
        if k >= 2:
            run_final(k - 2)
    run_stage2(CHUNKS - 1)
    run_final(CHUNKS - 2)
    run_final(CHUNKS - 1)
    for k in range(CHUNKS):
        run_forward(k)
    for k in range(CHUNKS):
        sib = o_part(cx, 1 - core, k)
        rdma(sib, sib, os_s.at[k], os_r.at[k], sibling).wait_recv()
        store_out(cx, 1 - core, k, 2).start()
    for k in range(CHUNKS):
        far = o_part(1 - cx, 1 - core, k)
        rdma(far, far, of_s.at[k], of_r.at[k], sibling).wait_recv()
        store_out(1 - cx, 1 - core, k, 3).start()

    ctx_cp.wait_send()
    m_cp.wait_send()
    ish_cp.wait_send()
    for cp in u_cps:
        cp.wait_send()
    for cp in fwd:
        cp.wait_send()
    for e in range(EXPERTS):
        rdma(in_part(e, core), in_part(e, core), in_s.at[e], in_r.at[e], sibling).wait_send()
    for k in range(CHUNKS):
        for cp in stage1(k):
            cp.wait_send()
        stage2(k).wait_send()
        mine = o_part(cx, core, k)
        theirs = o_part(1 - cx, core, k)
        rdma(mine, mine, os_s.at[k], os_r.at[k], sibling).wait_send()
        rdma(mine, mine, ox_s.at[k], ox_r.at[k], x_nbr).wait_send()
        rdma(theirs, theirs, of_s.at[k], of_r.at[k], sibling).wait_send()
        store_out(cx, core, k, 0).wait()
        store_out(1 - cx, core, k, 1).wait()
        store_out(cx, 1 - core, k, 2).wait()
        store_out(1 - cx, 1 - core, k, 3).wait()


def moe(ctx, routes, gain, hidden, w_o, sg, su, sd, wg, wu, wd):
    any_spec = pl.BlockSpec(memory_space=pl.ANY)
    vmem_spec = pl.BlockSpec(memory_space=pltpu.VMEM)
    dma = pltpu.SemaphoreType.DMA
    return pl.pallas_call(
        moe_kernel,
        out_shape=jax.ShapeDtypeStruct(hidden.shape, BF16),
        in_specs=[vmem_spec] * 3 + [any_spec] * 8,
        out_specs=any_spec,
        scratch_shapes=[
            pltpu.VMEM((RING, DIM, 512), BF16),
            pltpu.VMEM((ROWS, HALF), BF16),
            pltpu.VMEM((ROWS, HALF), BF16),
            pltpu.VMEM((2, ROWS, HALF), BF16),
            pltpu.VMEM((4, ROWS, DIM), BF16),
            pltpu.VMEM((2, ROWS, 512), BF16),
            pltpu.VMEM((ROWS, HALF), F32),
            pltpu.VMEM((2, 16, 2 * ROWS), F32),
            pltpu.VMEM((4, EXPERTS * SLOTS, ROWS), BF16),
            pltpu.VMEM((4, 3 * ROWS, EXPERTS * SLOTS), BF16),
            pltpu.VMEM((EXPERTS, 4 * SLOTS, DIM), BF16),
            pltpu.VMEM((EXPERTS, 4 * SLOTS, 1024), BF16),
            pltpu.VMEM((4, EXPERTS * SLOTS, CW), BF16),
            pltpu.VMEM((CHUNKS, 4, ROWS, CW), F32),
            pltpu.VMEM((CHUNKS, 2, ROWS, CW), F32),
            pltpu.VMEM((CHUNKS, ROWS, CW), F32),
            pltpu.VMEM((CHUNKS, ROWS, CW), F32),
            pltpu.VMEM((2, 2, CHUNKS, ROWS, CW), BF16),
            dma((RING,)), dma, dma((4,)), dma((4,)),
            dma((3,)), dma((3,)), dma((3,)), dma((3,)),
            dma((EXPERTS,)), dma((EXPERTS,)),
            dma((CHUNKS, 2)), dma((CHUNKS, 2)), dma((CHUNKS,)), dma((CHUNKS,)),
            dma((CHUNKS,)), dma((CHUNKS,)), dma((CHUNKS,)), dma((CHUNKS,)), dma((CHUNKS,)), dma((CHUNKS,)),
            dma((4, CHUNKS)),
        ],
        compiler_params=pltpu.CompilerParams(vmem_limit_bytes=62 * 1024 * 1024, collective_id=0, has_side_effects=True),
        name='experts',
    )(ctx, routes, gain, hidden, w_o, sg, su, sd, wg, wu, wd)


def solution(mesh):
    batch_spec = P(('inst', 'dev'))
    layer_batch = P(None, ('inst', 'dev'))
    expert_spec = P(None, 'dev')

    def device_fn(hidden, k_cache, v_cache, cache_lens, expert_ids, route_gates, attn_gain, ffn_gain, w_q, w_kv, w_o, shared_gate, shared_up, shared_down, w_gate, w_up, w_down):
        routes = jnp.concatenate([expert_ids[0].astype(F32).T, route_gates[0].T], axis=0)
        ctx = attention(hidden, cache_lens, attn_gain, w_q, w_kv, k_cache, v_cache)
        return moe(ctx, routes, ffn_gain, hidden, w_o, shared_gate, shared_up, shared_down, w_gate, w_up, w_down)

    in_specs = (batch_spec, layer_batch, layer_batch, batch_spec, layer_batch, layer_batch, P(), P(), P(), P(), P(), P(), P(), P(), expert_spec, expert_spec, expert_spec)
    return jax.shard_map(device_fn, mesh=mesh, in_specs=in_specs, out_specs=batch_spec, check_vma=False)
```

```python
import functools

import numpy as np
import jax
import jax.numpy as jnp
from jax import lax
from jax.experimental import pallas as pl
from jax.experimental.pallas import tpu as pltpu
from jax.sharding import PartitionSpec as P

NORM_EPS = 1e-6
ROPE_BASE = 10000.0
MESH = pl.DeviceIdType.MESH
LAST_DIMS = (((1,), (1,)), ((), ()))
F32 = jnp.float32
BF16 = jnp.bfloat16

ROWS = 128
HEADS = 8
HD = 128
DIM = 2048
HALF = DIM // 2
GROUP = 8
KV_RING = 8
RING = 16
QW = 512
LAYER = 0
S_CTX, S_IDS, S_M, S_IN, S_GATES = range(5)
X_LINK, Y_LINK, RELAY = range(3)
EXPERTS = 16
SLOTS = 32
CHUNKS = 4
CW = HALF // CHUNKS
ROWS_Y = 96


def norm_rows(rows_f, gain):
    inv_rms = lax.rsqrt(jnp.mean(rows_f * rows_f, axis=-1, keepdims=True) + NORM_EPS)
    return (rows_f * inv_rms * gain).astype(BF16)


def attn_kernel(lens_ref, hidden_ref, gain_ref, freq_ref, wq_ref, wkv_ref, kc_ref, vc_ref, ctx_ref,
                xbuf, wbuf, pos_buf, qbuf, nkbuf, nvbuf, cbuf, sbuf, pbuf, kbuf, vbuf, xsem, wsem, ksem, vsem):
    side = lax.axis_index('side')
    row0 = (side // 2) * ROWS
    core = side % 2
    h0 = core * HEADS
    groups = ROWS // GROUP

    def size_of(tok):
        return (lens_ref[row0 + tok] + 15) & -16

    def v_size_of(tok):
        return jnp.where(tok < KV_RING * GROUP, HD, size_of(tok))

    def start_group(grp):
        slot = grp & (KV_RING - 1)
        for i in range(GROUP):
            tok = grp * GROUP + i
            for src, dst, sem, size in ((kc_ref, kbuf, ksem, size_of), (vc_ref, vbuf, vsem, v_size_of)):
                size = pl.multiple_of(size(tok), 16)
                pltpu.make_async_copy(src.at[LAYER, row0 + tok, pl.ds(h0, HEADS), pl.ds(0, size), :],
                                      dst.at[slot, :, pl.ds(i * HD, size), :], sem.at[slot]).start()

    def wait_group(grp, buf, sem):
        slot = grp & (KV_RING - 1)
        size = size_of if buf is kbuf else v_size_of
        total = sum(size(grp * GROUP + i) for i in range(GROUP))
        whole = buf.at[slot, :, pl.ds(0, pl.multiple_of(total, 16)), :]
        pltpu.make_async_copy(whole, whole, sem.at[slot]).wait()

    x_cp = pltpu.make_async_copy(hidden_ref.at[pl.ds(row0, ROWS), :], xbuf, xsem)
    x_cp.start()
    w_cps = []
    for i in range(6):
        kind, j = i // 2, i % 2
        col = core * HALF + j * QW
        if kind == 0:
            src = wq_ref.at[LAYER, :, pl.ds(col, QW)]
        else:
            src = wkv_ref.at[LAYER, :, pl.ds((kind - 1) * DIM + col, QW)]
        cp = pltpu.make_async_copy(src, wbuf.at[i], wsem.at[i])
        cp.start()
        w_cps.append(cp)

    def fill_pos(i, carry):
        for r in range(8):
            row = i * 8 + r
            pos_buf[pl.ds(row, 1), :] = jnp.full((1, HD), lens_ref[row0 + row].astype(F32), F32)
        return carry
    lax.fori_loop(0, ROWS // 8, fill_pos, 0)
    angles = pos_buf[...] * freq_ref[...]
    cosine = jnp.cos(angles)
    lane = lax.broadcasted_iota(jnp.int32, (ROWS, HD), 1)
    sine = jnp.sin(angles)
    sine = jnp.where(lane < HD // 2, -sine, sine)

    x_cp.wait()
    normed = norm_rows(xbuf[...].astype(F32), gain_ref[...])
    lax.fori_loop(0, 3, lambda g, c: (start_group(g), c)[1], 0)
    for i in range(6):
        kind, j = i // 2, i % 2
        w_cps[i].wait()
        res = jnp.dot(normed, wbuf[i], preferred_element_type=F32).astype(BF16).astype(F32)
        for hh in range(4):
            h = j * 4 + hh
            val = res[:, hh * HD:(hh + 1) * HD]
            if kind < 2:
                val = (val * cosine + pltpu.roll(val, HD // 2, 1) * sine).astype(BF16).astype(F32)
            (qbuf, nkbuf, nvbuf)[kind][:, h * HD:(h + 1) * HD] = val
        if i == 1:
            lax.fori_loop(3, KV_RING, lambda g, c: (start_group(g), c)[1], 0)

    row_id = lax.broadcasted_iota(jnp.int32, (2 * GROUP, HD), 0) & (GROUP - 1)
    lane_f = lax.broadcasted_iota(jnp.int32, (GROUP, HD), 1).astype(F32)

    def rows_of(grp):
        return pl.ds(pl.multiple_of(grp * GROUP, GROUP), GROUP)

    def pair_of(ref, rows, hp):
        return jnp.concatenate([ref[rows, (2 * hp + p) * HD:(2 * hp + p + 1) * HD] for p in range(2)], axis=0)

    def score_group(grp):
        slot = grp & (KV_RING - 1)
        rows = rows_of(grp)
        valid = lane_f < pos_buf[rows, :]
        valid = jnp.concatenate([valid, valid], axis=0)
        for hp in range(HEADS // 2):
            zero = jnp.zeros((GROUP, HD), F32)
            first = jnp.concatenate([qbuf[rows, 2 * hp * HD:(2 * hp + 1) * HD], zero], axis=0)
            second = jnp.concatenate([zero, qbuf[rows, (2 * hp + 1) * HD:(2 * hp + 2) * HD]], axis=0)
            lhs = jnp.concatenate([first, second], axis=1).astype(BF16)
            rhs = jnp.concatenate([kbuf[slot, 2 * hp], kbuf[slot, 2 * hp + 1]], axis=1)
            full = lax.dot_general(lhs, rhs, LAST_DIMS, preferred_element_type=F32)
            sc = full[:, 0:HD]
            for i in range(1, GROUP):
                sc = jnp.where(row_id == i, full[:, i * HD:(i + 1) * HD], sc)
            sbuf[grp & 1, hp] = jnp.where(valid, sc * (HD ** -0.5), -jnp.inf)

    def soften_group(grp):
        rows = rows_of(grp)
        for hp in range(HEADS // 2):
            sc = sbuf[grp & 1, hp]
            self_sc = jnp.sum(pair_of(qbuf, rows, hp) * pair_of(nkbuf, rows, hp), axis=-1, keepdims=True) * (HD ** -0.5)
            peak = jnp.maximum(jnp.max(sc, axis=-1, keepdims=True), self_sc)
            wts = jnp.exp(sc - peak)
            self_w = jnp.exp(self_sc - peak)
            denom = jnp.sum(wts, axis=-1, keepdims=True) + self_w
            prob = wts / denom
            self_p = (self_w / denom).astype(BF16).astype(F32)
            wide = jnp.concatenate([jnp.where(row_id == i, prob, 0.0) for i in range(GROUP)], axis=1).astype(BF16)
            pbuf[grp & 1, hp] = wide
            for p in range(2):
                cols = slice((2 * hp + p) * HD, (2 * hp + p + 1) * HD)
                cbuf[rows, cols] = self_p[p * GROUP:(p + 1) * GROUP] * nvbuf[rows, cols]

    def value_group(grp):
        slot = grp & (KV_RING - 1)
        rows = rows_of(grp)
        for hp in range(HEADS // 2):
            rhs = jnp.concatenate([vbuf[slot, 2 * hp], vbuf[slot, 2 * hp + 1]], axis=1)
            ctx = jnp.dot(pbuf[grp & 1, hp], rhs, preferred_element_type=F32)
            for p in range(2):
                cols = slice((2 * hp + p) * HD, (2 * hp + p + 1) * HD)
                cbuf[rows, cols] += ctx[p * GROUP:(p + 1) * GROUP, p * HD:(p + 1) * HD]

    last = groups - 1
    wait_group(jnp.int32(0), kbuf, ksem)
    score_group(jnp.int32(0))
    wait_group(jnp.int32(1), kbuf, ksem)
    soften_group(jnp.int32(0))
    score_group(jnp.int32(1))

    def body(grp, carry):
        wait_group(grp - 1, vbuf, vsem)
        wait_group(grp + 1, kbuf, ksem)
        value_group(grp - 1)
        soften_group(grp)
        score_group(grp + 1)

        @pl.when(grp - 1 + KV_RING < groups)
        def _():
            start_group(grp - 1 + KV_RING)
        return carry
    lax.fori_loop(1, last, body, 0)
    wait_group(jnp.int32(last - 1), vbuf, vsem)
    wait_group(jnp.int32(last), vbuf, vsem)
    value_group(jnp.int32(last - 1))
    soften_group(jnp.int32(last))
    value_group(jnp.int32(last))
    ctx_ref[...] = cbuf[...].astype(BF16)


def attention(hidden, lens, gain, w_q, w_kv, k_cache, v_cache):
    freq = ROPE_BASE ** (-np.arange(HD // 2, dtype=np.float64) * 2.0 / HD)
    freq = np.concatenate([freq, freq])[None, :].astype(np.float32)
    any_spec = pl.BlockSpec(memory_space=pl.ANY)
    vmem_spec = pl.BlockSpec(memory_space=pltpu.VMEM)
    return pl.pallas_call(
        attn_kernel,
        out_shape=jax.ShapeDtypeStruct((ROWS, HALF), BF16),
        in_specs=[pl.BlockSpec(memory_space=pltpu.SMEM), any_spec, vmem_spec, vmem_spec] + [any_spec] * 4,
        out_specs=vmem_spec,
        scratch_shapes=[
            pltpu.VMEM((ROWS, DIM), BF16),
            pltpu.VMEM((6, DIM, QW), BF16),
            pltpu.VMEM((ROWS, HD), F32),
            pltpu.VMEM((ROWS, HALF), F32),
            pltpu.VMEM((ROWS, HALF), F32),
            pltpu.VMEM((ROWS, HALF), F32),
            pltpu.VMEM((ROWS, HALF), F32),
            pltpu.VMEM((2, HEADS // 2, 2 * GROUP, HD), F32),
            pltpu.VMEM((2, HEADS // 2, 2 * GROUP, GROUP * HD), BF16),
            pltpu.VMEM((KV_RING, HEADS, GROUP * HD, HD), BF16),
            pltpu.VMEM((KV_RING, HEADS, GROUP * HD, HD), BF16),
            pltpu.SemaphoreType.DMA,
            pltpu.SemaphoreType.DMA((6,)),
            pltpu.SemaphoreType.DMA((KV_RING,)),
            pltpu.SemaphoreType.DMA((KV_RING,)),
        ],
        compiler_params=pltpu.CompilerParams(vmem_limit_bytes=60 * HALF * HALF),
        name='attend',
    )(lens, hidden, gain, jnp.asarray(freq), w_q, w_kv, k_cache, v_cache)


def moe_kernel(gain_ref, ctx_ref, ids_ref, gates_ref, hidden_ref, wo_ref, sg_ref, su_ref, sd_ref, wg_ref, wu_ref, wd_ref, out_ref,
               ring, ctx_own, ctx_sib, xbuf, mbuf, uall, ish, base, ids_all, gates_all, dmat, cg, xe, inner, ybuf, pbuf,
               recv1, send2, recv2, oall,
               ring_sem, x_sem, misc_s, misc_r, u_s, u_r, uf_s, uf_r, in_s, in_r, p1_s, p1_r, p2_s, p2_r,
               os_s, os_r, ox_s, ox_r, of_s, of_r, out_sem):
    inst = lax.axis_index('inst')
    dy = lax.axis_index('dev')
    side = lax.axis_index('side')
    cx = side // 2
    core = side % 2
    blk0 = dy * 2 + cx
    col0 = core * HALF

    def dev_of(y, x, c):
        return (inst, y, x * 2 + c)
    sibling = dev_of(dy, cx, 1 - core)
    x_nbr = dev_of(dy, 1 - cx, core)
    y_nbr = dev_of(1 - dy, cx, core)

    def rdma(src, dst, s_sem, r_sem, dev):
        return pltpu.make_async_remote_copy(src_ref=src, dst_ref=dst, send_sem=s_sem, recv_sem=r_sem,
                                            device_id=dev, device_id_type=MESH)

    def start_wo(j):
        pltpu.make_async_copy(wo_ref.at[LAYER, :, pl.ds(col0 + j * QW, QW)], ring.at[j], ring_sem.at[j]).start()

    def start_gate(e, slot):
        pltpu.make_async_copy(wg_ref.at[LAYER, cx * EXPERTS + e, :, pl.ds(core * QW, QW)], ring.at[slot], ring_sem.at[slot]).start()

    def start_up(e, slot):
        pltpu.make_async_copy(wu_ref.at[LAYER, cx * EXPERTS + e, :, pl.ds(core * QW, QW)], ring.at[slot], ring_sem.at[slot]).start()

    def start_down(m, slot):
        k = m >> 2
        g = m & 3
        for i in range(4):
            pltpu.make_async_copy(wd_ref.at[LAYER, cx * EXPERTS + g * 4 + i, :, pl.ds(col0 + k * CW, CW)],
                                  ring.at[slot, pl.ds((i // 2) * HALF, HALF), pl.ds((i % 2) * CW, CW)],
                                  ring_sem.at[slot]).start()

    def wait_slot(slot):
        pltpu.make_async_copy(wg_ref.at[LAYER, 0, :, pl.ds(0, QW)], ring.at[slot], ring_sem.at[slot]).wait()

    def start_gu_block(b):
        e, up = (b - 5) // 2, (b - 5) % 2
        (start_up if up else start_gate)(e, b % RING)

    ctx_in = pltpu.make_async_copy(ctx_ref, ctx_own, x_sem.at[0])
    ctx_in.start()
    start_wo(0)
    start_wo(1)
    x_cp = pltpu.make_async_copy(hidden_ref.at[pl.ds(cx * ROWS, ROWS), pl.ds(col0, HALF)], xbuf, x_sem.at[1])
    x_cp.start()

    barrier = pltpu.get_barrier_semaphore()
    for dev in (sibling, x_nbr, y_nbr):
        pl.semaphore_signal(barrier, inc=1, device_id=dev, device_id_type=MESH)
    pltpu.make_async_copy(sg_ref.at[LAYER, :, pl.ds(core * QW, QW)], ring.at[2], ring_sem.at[2]).start()
    pltpu.make_async_copy(su_ref.at[LAYER, :, pl.ds(core * QW, QW)], ring.at[3], ring_sem.at[3]).start()
    ids_in = pltpu.make_async_copy(ids_ref, ids_all.at[dy], x_sem.at[2])
    gates_in = pltpu.make_async_copy(gates_ref, gates_all.at[dy], x_sem.at[3])
    ids_in.start()
    gates_in.start()
    pl.semaphore_wait(barrier, 3)

    ctx_in.wait()
    ctx_cp = rdma(ctx_own, ctx_sib, misc_s.at[S_CTX], misc_r.at[S_CTX], sibling)
    ctx_cp.start()

    own_row = core * HALF
    sib_row = (1 - core) * HALF
    wait_slot(0)
    wait_slot(1)
    for j in range(2):
        pltpu.make_async_copy(sd_ref.at[LAYER, :, pl.ds(col0 + j * QW, QW)], ring.at[4, pl.ds(j * HALF, HALF), :],
                              ring_sem.at[4]).start()
    for b in range(5, 9):
        start_gu_block(b)
    x_cp.wait()
    ctx_val = ctx_own[...]
    accs = [jnp.dot(ctx_val, ring[j, pl.ds(own_row, HALF), :], preferred_element_type=F32) for j in range(2)]
    ctx_cp.wait_recv()
    ctx_val = ctx_sib[...]
    for j in range(2):
        acc = accs[j] + jnp.dot(ctx_val, ring[j, pl.ds(sib_row, HALF), :], preferred_element_type=F32)
        mbuf[core, :, j * QW:(j + 1) * QW] = (xbuf[:, j * QW:(j + 1) * QW].astype(F32) + acc).astype(BF16)
    m_cp = rdma(mbuf.at[core], mbuf.at[core], misc_s.at[S_M], misc_r.at[S_M], sibling)
    m_cp.start()
    for b in range(9, 18):
        start_gu_block(b)
    m_other = rdma(mbuf.at[1 - core], mbuf.at[1 - core], misc_s.at[S_M], misc_r.at[S_M], sibling)
    m_other.wait_recv()
    m_lo = mbuf[0].astype(F32)
    m_hi = mbuf[1].astype(F32)
    total = jnp.sum(m_lo * m_lo, axis=-1, keepdims=True) + jnp.sum(m_hi * m_hi, axis=-1, keepdims=True)
    inv_rms = lax.rsqrt(total / DIM + NORM_EPS)
    uall[blk0, :, 0:HALF] = (m_lo * inv_rms * gain_ref[:, 0:HALF]).astype(BF16)
    uall[blk0, :, HALF:DIM] = (m_hi * inv_rms * gain_ref[:, HALF:DIM]).astype(BF16)

    blk_x = dy * 2 + 1 - cx
    blk_y = (1 - dy) * 2 + cx
    blk_d = (1 - dy) * 2 + 1 - cx

    def u_part(b, c, h):
        return uall.at[b, pl.ds(c * 64 + h * 32, 32), :]

    def u_copy(b, h, which, dev):
        return rdma(u_part(b, core, h), u_part(b, core, h), u_s.at[which, h], u_r.at[which, h], dev)

    def u_fwd(b, c, which, h):
        return rdma(u_part(b, c, h), u_part(b, c, h), uf_s.at[which, h], uf_r.at[which, h], sibling)
    u_copy(blk0, 0, X_LINK, x_nbr).start()
    u_copy(blk0, 1, Y_LINK, y_nbr).start()
    u_copy(blk0, 1, X_LINK, x_nbr).start()
    u_copy(blk0, 0, Y_LINK, y_nbr).start()
    ids_in.wait()
    gates_in.wait()
    ids_cp = rdma(ids_all.at[dy], ids_all.at[dy], misc_s.at[S_IDS], misc_r.at[S_IDS], y_nbr)
    gates_cp = rdma(gates_all.at[dy], gates_all.at[dy], misc_s.at[S_GATES], misc_r.at[S_GATES], y_nbr)
    ids_cp.start()
    gates_cp.start()

    wait_slot(2)
    wait_slot(3)
    u_own = uall[blk0]
    gate = jnp.dot(u_own, ring[2], preferred_element_type=F32)
    up = jnp.dot(u_own, ring[3], preferred_element_type=F32)
    ish[core] = (jax.nn.silu(gate) * up).astype(BF16)
    ish_cp = rdma(ish.at[core], ish.at[core], misc_s.at[S_IN], misc_r.at[S_IN], sibling)
    ish_cp.start()
    start_gu_block(18)
    start_gu_block(19)

    expert_id = dy * 32 + cx * EXPERTS + lax.broadcasted_iota(jnp.int32, (EXPERTS, ROWS), 0)
    before = (lax.broadcasted_iota(jnp.int32, (ROWS, ROWS), 0) < lax.broadcasted_iota(jnp.int32, (ROWS, ROWS), 1))
    before = jnp.where(before, 1.0, 0.0).astype(BF16)
    slot_id = lax.broadcasted_iota(jnp.int32, (SLOTS, ROWS), 0).astype(F32)

    def route_block(yb, xb):
        b = yb * 2 + xb
        hit = jnp.zeros((EXPERTS, ROWS), F32)
        wts = jnp.zeros((EXPERTS, ROWS), F32)
        for j in range(8):
            same = ids_all[yb, j:j + 1, xb * ROWS:(xb + 1) * ROWS] == expert_id
            hit = jnp.where(same, 1.0, hit)
            wts = jnp.where(same, gates_all[yb, j:j + 1, xb * ROWS:(xb + 1) * ROWS], wts)
        place = jnp.dot(hit.astype(BF16), before, preferred_element_type=F32)
        place = jnp.where(hit > 0.5, place, -1.0)
        pieces = []
        for e in range(EXPERTS):
            match = place[e:e + 1, :] == slot_id
            dmat[b, e * SLOTS:(e + 1) * SLOTS, :] = jnp.where(match, 1.0, 0.0).astype(BF16)
            pieces.append(jnp.where(match, wts[e:e + 1, :], 0.0))
        for q in range(4):
            part = jnp.concatenate(pieces[q * 4:(q + 1) * 4], axis=0).T
            high = part.astype(BF16)
            rest = part - high.astype(F32)
            mid = rest.astype(BF16)
            low = (rest - mid.astype(F32)).astype(BF16)
            cg[b, 0:ROWS, q * ROWS:(q + 1) * ROWS] = high
            cg[b, ROWS:256, q * ROWS:(q + 1) * ROWS] = mid
            cg[b, 256:384, q * ROWS:(q + 1) * ROWS] = low

    for xb in range(2):
        route_block(dy, xb)

    def dispatch(b):
        def one(n, carry):
            cols = pl.ds(pl.multiple_of(n * QW, QW), QW)
            rows = jnp.dot(dmat[b], uall[b, :, cols], preferred_element_type=F32).astype(BF16)
            for e in range(EXPERTS):
                xe[e, pl.ds(pl.multiple_of(b * SLOTS, SLOTS), SLOTS), cols] = rows[e * SLOTS:(e + 1) * SLOTS, :]
            return carry
        lax.fori_loop(0, DIM // QW, one, 0)

    u_copy(blk_x, 0, X_LINK, x_nbr).wait_recv()
    u_copy(blk_x, 0, RELAY, y_nbr).start()
    u_fwd(blk_x, core, X_LINK, 0).start()
    u_copy(blk_y, 1, Y_LINK, y_nbr).wait_recv()
    u_copy(blk_y, 1, RELAY, x_nbr).start()
    u_fwd(blk_y, core, Y_LINK, 1).start()

    rdma(ish.at[1 - core], ish.at[1 - core], misc_s.at[S_IN], misc_r.at[S_IN], sibling).wait_recv()
    wait_slot(4)
    for j in range(2):
        acc = jnp.dot(ish[0], ring[4, j * HALF:j * HALF + QW, :], preferred_element_type=F32)
        acc = acc + jnp.dot(ish[1], ring[4, j * HALF + QW:(j + 1) * HALF, :], preferred_element_type=F32)
        base[:, j * QW:(j + 1) * QW] = mbuf[core, :, j * QW:(j + 1) * QW].astype(F32) + acc.astype(BF16).astype(F32)
    start_gu_block(20)
    dispatch(blk0)
    rdma(ids_all.at[1 - dy], ids_all.at[1 - dy], misc_s.at[S_IDS], misc_r.at[S_IDS], y_nbr).wait_recv()
    rdma(gates_all.at[1 - dy], gates_all.at[1 - dy], misc_s.at[S_GATES], misc_r.at[S_GATES], y_nbr).wait_recv()
    u_copy(blk_x, 1, X_LINK, x_nbr).wait_recv()
    u_fwd(blk_x, core, X_LINK, 1).start()
    u_copy(blk_y, 0, Y_LINK, y_nbr).wait_recv()
    u_fwd(blk_y, core, Y_LINK, 0).start()
    for xb in range(2):
        route_block(1 - dy, xb)
    for h in range(2):
        u_fwd(blk_x, 1 - core, X_LINK, h).wait_recv()
    dispatch(blk_x)
    u_copy(blk_d, 0, RELAY, y_nbr).wait_recv()
    u_fwd(blk_d, core, RELAY, 0).start()
    u_copy(blk_d, 1, RELAY, x_nbr).wait_recv()
    u_fwd(blk_d, core, RELAY, 1).start()
    for h in range(2):
        u_fwd(blk_y, 1 - core, Y_LINK, h).wait_recv()
    dispatch(blk_y)
    for h in range(2):
        u_fwd(blk_d, 1 - core, RELAY, h).wait_recv()
    dispatch(blk_d)

    def in_part(e, c):
        return inner.at[e, :, pl.ds(pl.multiple_of(c * QW, QW), QW)]

    def in_copy(e, c):
        return rdma(in_part(e, c), in_part(e, c), in_s.at[e], in_r.at[e], sibling)

    def expert_pair(p, after):
        slots = [((5 + 4 * p + i) & (RING - 1)) for i in range(4)]
        for slot in slots:
            wait_slot(slot)
        for i in range(2):
            e = 2 * p + i
            rows = xe[e]
            gate = jnp.dot(rows, ring[slots[2 * i]], preferred_element_type=F32)
            up = jnp.dot(rows, ring[slots[2 * i + 1]], preferred_element_type=F32)
            inner[e, :, pl.ds(pl.multiple_of(core * QW, QW), QW)] = (jax.nn.silu(gate) * up).astype(BF16)
        for i in range(2):
            in_copy(2 * p + i, core).start()
        after(p, slots)

    def refill_experts(p, slots):
        for i in range(2):
            start_gate(2 * p + i + 8, slots[2 * i])
            start_up(2 * p + i + 8, slots[2 * i + 1])

    def refill_down(p, slots):
        for i in range(4):
            start_down(4 * (p - 4) + i, slots[i])

    lax.fori_loop(0, 4, lambda p, c: (expert_pair(p, refill_experts), c)[1], 0)
    lax.fori_loop(4, 8, lambda p, c: (expert_pair(p, refill_down), c)[1], 0)

    top = pl.ds(0, ROWS_Y)
    low = pl.ds(ROWS_Y, ROWS - ROWS_Y)

    def stage1(k, i):
        if i == 0:
            return [rdma(pbuf.at[k, blk_d, part, :], recv1.at[k, 0, part, :], p1_s.at[k, 0, a], p1_r.at[k, 0, a], dev)
                    for a, (part, dev) in enumerate(((top, y_nbr), (low, x_nbr)))]
        return [rdma(pbuf.at[k, b, part, :], recv1.at[k, 1, part, :], p1_s.at[k, 1, a], p1_r.at[k, 1, a], dev)
                for a, (b, part, dev) in enumerate(((blk_y, top, y_nbr), (blk_x, low, x_nbr)))]

    def stage2(k):
        return [rdma(send2.at[k, part, :], recv2.at[k, part, :], p2_s.at[k, a], p2_r.at[k, a], dev)
                for a, (part, dev) in enumerate(((top, x_nbr), (low, y_nbr)))]

    def run_stage2(k):
        first, second = stage1(k, 0)
        going = stage2(k)
        first.wait_recv()
        send2[k, 0:ROWS_Y, :] = pbuf[k, blk_x, 0:ROWS_Y, :] + recv1[k, 0, 0:ROWS_Y, :]
        going[0].start()
        second.wait_recv()
        send2[k, ROWS_Y:ROWS, :] = pbuf[k, blk_y, ROWS_Y:ROWS, :] + recv1[k, 0, ROWS_Y:ROWS, :]
        going[1].start()

    def o_part(x, c, k):
        return oall.at[x, c, k]

    def store_out(x, c, k, which):
        return pltpu.make_async_copy(o_part(x, c, k),
                                     out_ref.at[pl.ds(x * ROWS, ROWS), pl.ds(pl.multiple_of(c * HALF + k * CW, CW), CW)],
                                     out_sem.at[which, k])

    def o_sib(k, c):
        return rdma(o_part(cx, c, k), o_part(cx, c, k), os_s.at[k], os_r.at[k], sibling)

    def o_x(k, x):
        return rdma(o_part(x, core, k), o_part(x, core, k), ox_s.at[k], ox_r.at[k], x_nbr)

    def o_fwd(k, c):
        return rdma(o_part(1 - cx, c, k), o_part(1 - cx, c, k), of_s.at[k], of_r.at[k], sibling)

    def run_final(k):
        for cp in stage1(k, 1):
            cp.wait_recv()
        for cp in stage2(k):
            cp.wait_recv()
        routed = pbuf[k, blk0] + recv1[k, 1] + recv2[k]
        oall[cx, core, k] = (base[:, k * CW:(k + 1) * CW] + routed).astype(BF16)
        o_x(k, cx).start()
        o_sib(k, core).start()
        store_out(cx, core, k, 0).start()

    def run_forward(k):
        o_x(k, 1 - cx).wait_recv()
        o_fwd(k, core).start()
        store_out(1 - cx, core, k, 1).start()

    for e in range(EXPERTS):
        in_copy(e, 1 - core).wait_recv()

    for k in range(CHUNKS):
        def down_group(g, carry):
            slot = (5 + 4 * k + g) & (RING - 1)
            wait_slot(slot)
            for i in range(4):
                e = g * 4 + i
                w = ring[slot, (i // 2) * HALF:(i // 2 + 1) * HALF, (i % 2) * CW:(i % 2 + 1) * CW]
                res = jnp.dot(inner[e], w, preferred_element_type=F32).astype(BF16)
                for b in range(4):
                    ybuf[b, pl.ds(pl.multiple_of(e * SLOTS, SLOTS), SLOTS), :] = res[b * SLOTS:(b + 1) * SLOTS, :]
            return carry
        lax.fori_loop(0, 4, down_group, 0)

        def combine(b):
            res = jnp.dot(cg[b], ybuf[b], preferred_element_type=F32)
            pbuf[k, b] = res[0:ROWS] + res[ROWS:256] + res[256:384]
        combine(blk_d)
        for cp in stage1(k, 0):
            cp.start()
        combine(blk_y)
        combine(blk_x)
        for cp in stage1(k, 1):
            cp.start()
        combine(blk0)
        if k >= 1:
            run_stage2(k - 1)
        if k >= 2:
            run_final(k - 2)
    run_stage2(CHUNKS - 1)
    run_final(CHUNKS - 2)
    for k in range(CHUNKS - 1):
        run_forward(k)
    run_final(CHUNKS - 1)
    run_forward(CHUNKS - 1)
    for k in range(CHUNKS):
        o_sib(k, 1 - core).wait_recv()
        store_out(cx, 1 - core, k, 2).start()
    for k in range(CHUNKS):
        o_fwd(k, 1 - core).wait_recv()
        store_out(1 - cx, 1 - core, k, 3).start()

    for cp in (ctx_cp, m_cp, ids_cp, gates_cp, ish_cp):
        cp.wait_send()
    for h in range(2):
        u_copy(blk0, h, X_LINK, x_nbr).wait_send()
        u_copy(blk0, h, Y_LINK, y_nbr).wait_send()
        u_fwd(blk_x, core, X_LINK, h).wait_send()
        u_fwd(blk_y, core, Y_LINK, h).wait_send()
        u_fwd(blk_d, core, RELAY, h).wait_send()
    u_copy(blk_x, 0, RELAY, y_nbr).wait_send()
    u_copy(blk_y, 1, RELAY, x_nbr).wait_send()
    for e in range(EXPERTS):
        in_copy(e, core).wait_send()
    for k in range(CHUNKS):
        for cp in stage1(k, 0) + stage1(k, 1) + stage2(k):
            cp.wait_send()
        o_sib(k, core).wait_send()
        o_x(k, cx).wait_send()
        o_fwd(k, core).wait_send()
        store_out(cx, core, k, 0).wait()
        store_out(1 - cx, core, k, 1).wait()
        store_out(cx, 1 - core, k, 2).wait()
        store_out(1 - cx, 1 - core, k, 3).wait()


def moe(ctx, ids, gates, gain, hidden, w_o, sg, su, sd, wg, wu, wd):
    any_spec = pl.BlockSpec(memory_space=pl.ANY)
    vmem_spec = pl.BlockSpec(memory_space=pltpu.VMEM)
    dma = pltpu.SemaphoreType.DMA
    return pl.pallas_call(
        moe_kernel,
        out_shape=jax.ShapeDtypeStruct(hidden.shape, BF16),
        in_specs=[vmem_spec] + [any_spec] * 11,
        out_specs=any_spec,
        scratch_shapes=[
            pltpu.VMEM((RING, DIM, QW), BF16),
            pltpu.VMEM((ROWS, HALF), BF16),
            pltpu.VMEM((ROWS, HALF), BF16),
            pltpu.VMEM((ROWS, HALF), BF16),
            pltpu.VMEM((2, ROWS, HALF), BF16),
            pltpu.VMEM((4, ROWS, DIM), BF16),
            pltpu.VMEM((2, ROWS, QW), BF16),
            pltpu.VMEM((ROWS, HALF), F32),
            pltpu.VMEM((2, 8, 2 * ROWS), jnp.int32),
            pltpu.VMEM((2, 8, 2 * ROWS), F32),
            pltpu.VMEM((4, EXPERTS * SLOTS, ROWS), BF16),
            pltpu.VMEM((4, 3 * ROWS, EXPERTS * SLOTS), BF16),
            pltpu.VMEM((EXPERTS, 4 * SLOTS, DIM), BF16),
            pltpu.VMEM((EXPERTS, 4 * SLOTS, HALF), BF16),
            pltpu.VMEM((4, EXPERTS * SLOTS, CW), BF16),
            pltpu.VMEM((CHUNKS, 4, ROWS, CW), F32),
            pltpu.VMEM((CHUNKS, 2, ROWS, CW), F32),
            pltpu.VMEM((CHUNKS, ROWS, CW), F32),
            pltpu.VMEM((CHUNKS, ROWS, CW), F32),
            pltpu.VMEM((2, 2, CHUNKS, ROWS, CW), BF16),
            dma((RING,)), dma((4,)), dma((5,)), dma((5,)),
            dma((3, 2)), dma((3, 2)), dma((3, 2)), dma((3, 2)),
            dma((EXPERTS,)), dma((EXPERTS,)),
            dma((CHUNKS, 2, 2)), dma((CHUNKS, 2, 2)), dma((CHUNKS, 2)), dma((CHUNKS, 2)),
            dma((CHUNKS,)), dma((CHUNKS,)), dma((CHUNKS,)), dma((CHUNKS,)), dma((CHUNKS,)), dma((CHUNKS,)),
            dma((4, CHUNKS)),
        ],
        compiler_params=pltpu.CompilerParams(vmem_limit_bytes=60 * HALF * HALF, collective_id=0, has_side_effects=True),
        name='experts',
    )(gain, ctx, ids, gates, hidden, w_o, sg, su, sd, wg, wu, wd)


def solution(mesh):
    batch_spec = P(('inst', 'dev'))
    layer_batch = P(None, ('inst', 'dev'))
    expert_spec = P(None, 'dev')

    def device_fn(hidden, k_cache, v_cache, cache_lens, expert_ids, route_gates, attn_gain, ffn_gain, w_q, w_kv, w_o, shared_gate, shared_up, shared_down, w_gate, w_up, w_down):
        ctx = attention(hidden, cache_lens, attn_gain, w_q, w_kv, k_cache, v_cache)
        return moe(ctx, expert_ids[0].T, route_gates[0].T, ffn_gain, hidden, w_o, shared_gate, shared_up, shared_down, w_gate, w_up, w_down)

    in_specs = (batch_spec, layer_batch, layer_batch, batch_spec, layer_batch, layer_batch, P(), P(), P(), P(), P(), P(), P(), P(), expert_spec, expert_spec, expert_spec)
    return jax.shard_map(device_fn, mesh=mesh, in_specs=in_specs, out_specs=batch_spec, check_vma=False)
```

```python
import functools

import numpy as np
import jax
import jax.numpy as jnp
from jax import lax
from jax.experimental import pallas as pl
from jax.experimental.pallas import tpu as pltpu
from jax.sharding import PartitionSpec as P

NORM_EPS = 1e-6
ROPE_BASE = 10000.0
MESH = pl.DeviceIdType.MESH
LAST_DIMS = (((1,), (1,)), ((), ()))
F32 = jnp.float32
BF16 = jnp.bfloat16

ROWS = 128
HEADS = 8
HD = 128
DIM = 2048
HALF = DIM // 2
HH = HEADS // 2
GROUP = 8
KV_RING = 8
PAIRS = ROWS // (2 * GROUP)
RING = 20
QW = 512
LAYER = 0
S_CTX, S_IDS, S_M, S_IN, S_GATES = range(5)
X_LINK, Y_LINK, RELAY = range(3)
XE = 8
EXPERTS = 16
SLOTS = 32
CHUNKS = 4
CW = HALF // CHUNKS
ROWS_Y = 96


def norm_rows(rows_f, gain):
    inv_rms = lax.rsqrt(jnp.mean(rows_f * rows_f, axis=-1, keepdims=True) + NORM_EPS)
    return (rows_f * inv_rms * gain).astype(BF16)


def attn_kernel(lens_ref, hidden_ref, gain_ref, freq_ref, wq_ref, wkv_ref, kc_ref, vc_ref, ctx_ref,
                xbuf, nbuf, cosbuf, sinbuf, wbuf, pos_buf, qbuf, nkbuf, nvbuf, cbuf, sbuf, pbuf, kbuf, vbuf, xsem, wsem, ksem, vsem):
    side = lax.axis_index('side')
    row0 = (side // 2) * ROWS
    core = side % 2
    h0 = core * HEADS

    def size_of(unit, tok):
        return (lens_ref[row0 + tok] + 15) & -16

    def v_size_of(unit, tok):
        return jnp.where(unit < KV_RING, HD, size_of(unit, tok))

    def first_token(unit, d):
        return (unit & (PAIRS - 1)) * (2 * GROUP) + d * GROUP

    def start_unit(unit):
        slot = unit & (KV_RING - 1)
        heads = pl.ds(h0 + (unit >> 3) * HH, HH)
        for d in range(2):
            for i in range(GROUP):
                tok = first_token(unit, d) + i
                for src, dst, sem, size in ((kc_ref, kbuf, ksem, size_of), (vc_ref, vbuf, vsem, v_size_of)):
                    size = pl.multiple_of(size(unit, tok), 16)
                    pltpu.make_async_copy(src.at[LAYER, row0 + tok, heads, pl.ds(0, size), :],
                                          dst.at[slot, pl.ds(d * HH, HH), pl.ds(i * HD, size), :], sem.at[slot, d]).start()

    def wait_unit(unit, buf, sem):
        slot = unit & (KV_RING - 1)
        size = size_of if buf is kbuf else v_size_of
        for d in range(2):
            total = sum(size(unit, first_token(unit, d) + i) for i in range(GROUP))
            whole = buf.at[slot, pl.ds(d * HH, HH), pl.ds(0, pl.multiple_of(total, 16)), :]
            pltpu.make_async_copy(whole, whole, sem.at[slot, d]).wait()

    x_cp = pltpu.make_async_copy(hidden_ref.at[pl.ds(row0, ROWS), :], xbuf, xsem)
    x_cp.start()

    def weight_copy(j, kind):
        col = core * HALF + j * QW
        if kind == 0:
            src = wq_ref.at[LAYER, :, pl.ds(col, QW)]
        else:
            src = wkv_ref.at[LAYER, :, pl.ds((kind - 1) * DIM + col, QW)]
        return pltpu.make_async_copy(src, wbuf.at[j * 3 + kind], wsem.at[j * 3 + kind])

    def start_units(lo, hi):
        lax.fori_loop(lo, hi, lambda u, c: (start_unit(u), c)[1], 0)
    for kind in range(3):
        weight_copy(0, kind).start()

    def fill_pos(i, carry):
        for r in range(8):
            row = i * 8 + r
            pos_buf[pl.ds(row, 1), :] = jnp.full((1, HD), lens_ref[row0 + row].astype(F32), F32)
        return carry
    lax.fori_loop(0, ROWS // 8, fill_pos, 0)
    angles = pos_buf[...] * freq_ref[...]
    cosine = jnp.cos(angles)
    lane = lax.broadcasted_iota(jnp.int32, (ROWS, HD), 1)
    sine = jnp.sin(angles)
    sine = jnp.where(lane < HD // 2, -sine, sine)

    start_units(0, 2)
    for kind in range(3):
        weight_copy(1, kind).start()
    x_cp.wait()
    nbuf[...] = norm_rows(xbuf[...].astype(F32), gain_ref[...])
    cosbuf[...] = cosine
    sinbuf[...] = sine
    start_units(2, KV_RING)

    def project(j):
        for kind in range(3):
            weight_copy(j, kind).wait()
            res = jnp.dot(nbuf[...], wbuf[j * 3 + kind], preferred_element_type=F32).astype(BF16).astype(F32)
            for hh in range(HH):
                h = j * HH + hh
                val = res[:, hh * HD:(hh + 1) * HD]
                if kind < 2:
                    val = (val * cosbuf[...] + pltpu.roll(val, HD // 2, 1) * sinbuf[...]).astype(BF16).astype(F32)
                (qbuf, nkbuf, nvbuf)[kind][:, h * HD:(h + 1) * HD] = val
    project(0)

    row_id = lax.broadcasted_iota(jnp.int32, (2 * GROUP, HD), 0) & (GROUP - 1)
    lane_f = lax.broadcasted_iota(jnp.int32, (GROUP, HD), 1).astype(F32)

    def parts_of(unit):
        for d in range(2):
            rows = pl.ds(pl.multiple_of(first_token(unit, d), GROUP), GROUP)
            for hp in range(2):
                head = (unit >> 3) * HH + 2 * hp
                cols = [pl.ds(pl.multiple_of((head + p) * HD, HD), HD) for p in range(2)]
                yield 2 * d + hp, d * HH + 2 * hp, rows, cols

    def score_unit(unit):
        slot = unit & (KV_RING - 1)
        zero = jnp.zeros((GROUP, HD), F32)
        for n, at, rows, cols in parts_of(unit):
            valid = lane_f < pos_buf[rows, :]
            valid = jnp.concatenate([valid, valid], axis=0)
            first = jnp.concatenate([qbuf[rows, cols[0]], zero], axis=0)
            second = jnp.concatenate([zero, qbuf[rows, cols[1]]], axis=0)
            lhs = jnp.concatenate([first, second], axis=1).astype(BF16)
            rhs = jnp.concatenate([kbuf[slot, at], kbuf[slot, at + 1]], axis=1)
            full = lax.dot_general(lhs, rhs, LAST_DIMS, preferred_element_type=F32)
            sc = full[:, 0:HD]
            for i in range(1, GROUP):
                sc = jnp.where(row_id == i, full[:, i * HD:(i + 1) * HD], sc)
            sbuf[unit & 1, n] = jnp.where(valid, sc * (HD ** -0.5), -jnp.inf)

    def soften_unit(unit):
        for n, at, rows, cols in parts_of(unit):
            sc = sbuf[unit & 1, n]
            q_k = [jnp.concatenate([ref[rows, c] for c in cols], axis=0) for ref in (qbuf, nkbuf)]
            self_sc = jnp.sum(q_k[0] * q_k[1], axis=-1, keepdims=True) * (HD ** -0.5)
            peak = jnp.maximum(jnp.max(sc, axis=-1, keepdims=True), self_sc)
            wts = jnp.exp(sc - peak)
            self_w = jnp.exp(self_sc - peak)
            denom = jnp.sum(wts, axis=-1, keepdims=True) + self_w
            prob = wts / denom
            self_p = (self_w / denom).astype(BF16).astype(F32)
            wide = jnp.concatenate([jnp.where(row_id == i, prob, 0.0) for i in range(GROUP)], axis=1).astype(BF16)
            pbuf[unit & 1, n] = wide
            for p in range(2):
                cbuf[rows, cols[p]] = self_p[p * GROUP:(p + 1) * GROUP] * nvbuf[rows, cols[p]]

    def value_unit(unit):
        slot = unit & (KV_RING - 1)
        for n, at, rows, cols in parts_of(unit):
            rhs = jnp.concatenate([vbuf[slot, at], vbuf[slot, at + 1]], axis=1)
            ctx = jnp.dot(pbuf[unit & 1, n], rhs, preferred_element_type=F32)
            for p in range(2):
                cbuf[rows, cols[p]] += ctx[p * GROUP:(p + 1) * GROUP, p * HD:(p + 1) * HD]

    last = 2 * PAIRS - 1
    wait_unit(jnp.int32(0), kbuf, ksem)
    score_unit(jnp.int32(0))
    wait_unit(jnp.int32(1), kbuf, ksem)
    soften_unit(jnp.int32(0))
    score_unit(jnp.int32(1))

    def body(unit, carry):
        wait_unit(unit - 1, vbuf, vsem)
        wait_unit(unit + 1, kbuf, ksem)
        value_unit(unit - 1)
        soften_unit(unit)
        score_unit(unit + 1)

        @pl.when(unit - 1 + KV_RING <= last)
        def _():
            start_unit(unit - 1 + KV_RING)
        return carry
    lax.fori_loop(1, PAIRS - 1, body, 0)
    project(1)
    lax.fori_loop(PAIRS - 1, last, body, 0)
    wait_unit(jnp.int32(last - 1), vbuf, vsem)
    wait_unit(jnp.int32(last), vbuf, vsem)
    value_unit(jnp.int32(last - 1))
    soften_unit(jnp.int32(last))
    value_unit(jnp.int32(last))
    ctx_ref[...] = cbuf[...].astype(BF16)


def attention(hidden, lens, gain, w_q, w_kv, k_cache, v_cache):
    freq = ROPE_BASE ** (-np.arange(HD // 2, dtype=np.float64) * 2.0 / HD)
    freq = np.concatenate([freq, freq])[None, :].astype(np.float32)
    any_spec = pl.BlockSpec(memory_space=pl.ANY)
    vmem_spec = pl.BlockSpec(memory_space=pltpu.VMEM)
    return pl.pallas_call(
        attn_kernel,
        out_shape=jax.ShapeDtypeStruct((ROWS, HALF), BF16),
        in_specs=[pl.BlockSpec(memory_space=pltpu.SMEM), any_spec, vmem_spec, vmem_spec] + [any_spec] * 4,
        out_specs=vmem_spec,
        scratch_shapes=[
            pltpu.VMEM((ROWS, DIM), BF16),
            pltpu.VMEM((ROWS, DIM), BF16),
            pltpu.VMEM((ROWS, HD), F32),
            pltpu.VMEM((ROWS, HD), F32),
            pltpu.VMEM((6, DIM, QW), BF16),
            pltpu.VMEM((ROWS, HD), F32),
            pltpu.VMEM((ROWS, HALF), F32),
            pltpu.VMEM((ROWS, HALF), F32),
            pltpu.VMEM((ROWS, HALF), F32),
            pltpu.VMEM((ROWS, HALF), F32),
            pltpu.VMEM((2, HEADS // 2, 2 * GROUP, HD), F32),
            pltpu.VMEM((2, HEADS // 2, 2 * GROUP, GROUP * HD), BF16),
            pltpu.VMEM((KV_RING, 2 * HH, GROUP * HD, HD), BF16),
            pltpu.VMEM((KV_RING, 2 * HH, GROUP * HD, HD), BF16),
            pltpu.SemaphoreType.DMA,
            pltpu.SemaphoreType.DMA((6,)),
            pltpu.SemaphoreType.DMA((KV_RING, 2)),
            pltpu.SemaphoreType.DMA((KV_RING, 2)),
        ],
        compiler_params=pltpu.CompilerParams(vmem_limit_bytes=60 * HALF * HALF),
        name='attend',
    )(lens, hidden, gain, jnp.asarray(freq), w_q, w_kv, k_cache, v_cache)


def moe_kernel(gain_ref, ctx_ref, ids_ref, gates_ref, hidden_ref, wo_ref, sg_ref, su_ref, sd_ref, wg_ref, wu_ref, wd_ref, out_ref,
               ring, ctx_own, ctx_sib, xbuf, mbuf, uall, ish, base, ids_all, gates_all, dmat, cg, xe, inner, ybuf, pbuf,
               recv1, send2, recv2, oall,
               ring_sem, x_sem, misc_s, misc_r, u_s, u_r, uf_s, uf_r, in_s, in_r, p1_s, p1_r, p2_s, p2_r,
               os_s, os_r, ox_s, ox_r, of_s, of_r, out_sem):
    inst = lax.axis_index('inst')
    dy = lax.axis_index('dev')
    side = lax.axis_index('side')
    cx = side // 2
    core = side % 2
    blk0 = dy * 2 + cx
    col0 = core * HALF

    def dev_of(y, x, c):
        return (inst, y, x * 2 + c)
    sibling = dev_of(dy, cx, 1 - core)
    x_nbr = dev_of(dy, 1 - cx, core)
    y_nbr = dev_of(1 - dy, cx, core)

    def rdma(src, dst, s_sem, r_sem, dev):
        return pltpu.make_async_remote_copy(src_ref=src, dst_ref=dst, send_sem=s_sem, recv_sem=r_sem,
                                            device_id=dev, device_id_type=MESH)

    def start_wo(j):
        pltpu.make_async_copy(wo_ref.at[LAYER, :, pl.ds(col0 + j * QW, QW)], ring.at[j], ring_sem.at[j]).start()

    def start_gate(e, slot):
        pltpu.make_async_copy(wg_ref.at[LAYER, cx * EXPERTS + e, :, pl.ds(core * QW, QW)], ring.at[slot], ring_sem.at[slot]).start()

    def start_up(e, slot):
        pltpu.make_async_copy(wu_ref.at[LAYER, cx * EXPERTS + e, :, pl.ds(core * QW, QW)], ring.at[slot], ring_sem.at[slot]).start()

    def start_down(m, slot):
        k = m >> 2
        g = m & 3
        for i in range(4):
            pltpu.make_async_copy(wd_ref.at[LAYER, cx * EXPERTS + g * 4 + i, :, pl.ds(col0 + k * CW, CW)],
                                  ring.at[slot, pl.ds((i // 2) * HALF, HALF), pl.ds((i % 2) * CW, CW)],
                                  ring_sem.at[slot]).start()

    def wait_slot(slot):
        pltpu.make_async_copy(wg_ref.at[LAYER, 0, :, pl.ds(0, QW)], ring.at[slot], ring_sem.at[slot]).wait()

    def start_gu_block(b):
        e, up = (b - 5) // 2, (b - 5) % 2
        (start_up if up else start_gate)(e, b % RING)

    ctx_in = pltpu.make_async_copy(ctx_ref, ctx_own, x_sem.at[0])
    ctx_in.start()
    start_wo(0)
    start_wo(1)
    x_cp = pltpu.make_async_copy(hidden_ref.at[pl.ds(cx * ROWS, ROWS), pl.ds(col0, HALF)], xbuf, x_sem.at[1])
    x_cp.start()

    barrier = pltpu.get_barrier_semaphore()
    for dev in (sibling, x_nbr, y_nbr):
        pl.semaphore_signal(barrier, inc=1, device_id=dev, device_id_type=MESH)
    pltpu.make_async_copy(sg_ref.at[LAYER, :, pl.ds(core * QW, QW)], ring.at[2], ring_sem.at[2]).start()
    pltpu.make_async_copy(su_ref.at[LAYER, :, pl.ds(core * QW, QW)], ring.at[3], ring_sem.at[3]).start()
    ids_in = pltpu.make_async_copy(ids_ref, ids_all.at[dy], x_sem.at[2])
    gates_in = pltpu.make_async_copy(gates_ref, gates_all.at[dy], x_sem.at[3])
    ids_in.start()
    gates_in.start()
    pl.semaphore_wait(barrier, 3)

    ctx_in.wait()
    ctx_cp = rdma(ctx_own, ctx_sib, misc_s.at[S_CTX], misc_r.at[S_CTX], sibling)
    ctx_cp.start()

    own_row = core * HALF
    sib_row = (1 - core) * HALF
    wait_slot(0)
    wait_slot(1)
    for j in range(2):
        pltpu.make_async_copy(sd_ref.at[LAYER, :, pl.ds(col0 + j * QW, QW)], ring.at[4, pl.ds(j * HALF, HALF), :],
                              ring_sem.at[4]).start()
    for b in range(5, 9):
        start_gu_block(b)
    x_cp.wait()
    ctx_val = ctx_own[...]
    accs = [jnp.dot(ctx_val, ring[j, pl.ds(own_row, HALF), :], preferred_element_type=F32) for j in range(2)]
    ctx_cp.wait_recv()
    ctx_val = ctx_sib[...]
    for j in range(2):
        acc = accs[j] + jnp.dot(ctx_val, ring[j, pl.ds(sib_row, HALF), :], preferred_element_type=F32)
        mbuf[core, :, j * QW:(j + 1) * QW] = (xbuf[:, j * QW:(j + 1) * QW].astype(F32) + acc).astype(BF16)
    m_cp = rdma(mbuf.at[core], mbuf.at[core], misc_s.at[S_M], misc_r.at[S_M], sibling)
    m_cp.start()
    for b in range(9, 22):
        start_gu_block(b)
    m_other = rdma(mbuf.at[1 - core], mbuf.at[1 - core], misc_s.at[S_M], misc_r.at[S_M], sibling)
    m_other.wait_recv()
    m_lo = mbuf[0].astype(F32)
    m_hi = mbuf[1].astype(F32)
    total = jnp.sum(m_lo * m_lo, axis=-1, keepdims=True) + jnp.sum(m_hi * m_hi, axis=-1, keepdims=True)
    inv_rms = lax.rsqrt(total / DIM + NORM_EPS)
    uall[blk0, :, 0:HALF] = (m_lo * inv_rms * gain_ref[:, 0:HALF]).astype(BF16)
    uall[blk0, :, HALF:DIM] = (m_hi * inv_rms * gain_ref[:, HALF:DIM]).astype(BF16)

    blk_x = dy * 2 + 1 - cx
    blk_y = (1 - dy) * 2 + cx
    blk_d = (1 - dy) * 2 + 1 - cx

    def u_part(b, c, h):
        return uall.at[b, pl.ds(c * 64 + h * 32, 32), :]

    def u_copy(b, h, which, dev):
        return rdma(u_part(b, core, h), u_part(b, core, h), u_s.at[which, h], u_r.at[which, h], dev)

    def u_fwd(b, c, which, h):
        return rdma(u_part(b, c, h), u_part(b, c, h), uf_s.at[which, h], uf_r.at[which, h], sibling)
    u_copy(blk0, 0, X_LINK, x_nbr).start()
    u_copy(blk0, 1, Y_LINK, y_nbr).start()
    u_copy(blk0, 1, X_LINK, x_nbr).start()
    u_copy(blk0, 0, Y_LINK, y_nbr).start()
    ids_in.wait()
    gates_in.wait()
    ids_cp = rdma(ids_all.at[dy], ids_all.at[dy], misc_s.at[S_IDS], misc_r.at[S_IDS], y_nbr)
    gates_cp = rdma(gates_all.at[dy], gates_all.at[dy], misc_s.at[S_GATES], misc_r.at[S_GATES], y_nbr)
    ids_cp.start()
    gates_cp.start()

    wait_slot(2)
    wait_slot(3)
    u_own = uall[blk0]
    gate = jnp.dot(u_own, ring[2], preferred_element_type=F32)
    up = jnp.dot(u_own, ring[3], preferred_element_type=F32)
    ish[core] = (jax.nn.silu(gate) * up).astype(BF16)
    ish_cp = rdma(ish.at[core], ish.at[core], misc_s.at[S_IN], misc_r.at[S_IN], sibling)
    ish_cp.start()
    start_gu_block(22)
    start_gu_block(23)

    expert_id = dy * 32 + cx * EXPERTS + lax.broadcasted_iota(jnp.int32, (EXPERTS, ROWS), 0)
    before = (lax.broadcasted_iota(jnp.int32, (ROWS, ROWS), 0) < lax.broadcasted_iota(jnp.int32, (ROWS, ROWS), 1))
    before = jnp.where(before, 1.0, 0.0).astype(BF16)
    slot_id = lax.broadcasted_iota(jnp.int32, (SLOTS, ROWS), 0).astype(F32)

    def route_block(yb, xb):
        b = yb * 2 + xb
        hit = jnp.zeros((EXPERTS, ROWS), F32)
        wts = jnp.zeros((EXPERTS, ROWS), F32)
        for j in range(8):
            same = ids_all[yb, j:j + 1, xb * ROWS:(xb + 1) * ROWS] == expert_id
            hit = jnp.where(same, 1.0, hit)
            wts = jnp.where(same, gates_all[yb, j:j + 1, xb * ROWS:(xb + 1) * ROWS], wts)
        place = jnp.dot(hit.astype(BF16), before, preferred_element_type=F32)
        place = jnp.where(hit > 0.5, place, -1.0)
        pieces = []
        for e in range(EXPERTS):
            match = place[e:e + 1, :] == slot_id
            dmat[b, e * SLOTS:(e + 1) * SLOTS, :] = jnp.where(match, 1.0, 0.0).astype(BF16)
            pieces.append(jnp.where(match, wts[e:e + 1, :], 0.0))
        for q in range(4):
            part = jnp.concatenate(pieces[q * 4:(q + 1) * 4], axis=0).T
            high = part.astype(BF16)
            rest = part - high.astype(F32)
            mid = rest.astype(BF16)
            low = (rest - mid.astype(F32)).astype(BF16)
            cg[b, 0:ROWS, q * ROWS:(q + 1) * ROWS] = high
            cg[b, ROWS:256, q * ROWS:(q + 1) * ROWS] = mid
            cg[b, 256:384, q * ROWS:(q + 1) * ROWS] = low

    for xb in range(2):
        route_block(dy, xb)

    half_rows = XE * SLOTS

    def dispatch(b, part):
        def one(n, carry):
            cols = pl.ds(pl.multiple_of(n * QW, QW), QW)
            rows = jnp.dot(dmat[b, part * half_rows:(part + 1) * half_rows, :], uall[b, :, cols],
                           preferred_element_type=F32).astype(BF16)
            for e in range(XE):
                xe[e, pl.ds(pl.multiple_of(b * SLOTS, SLOTS), SLOTS), cols] = rows[e * SLOTS:(e + 1) * SLOTS, :]
            return carry
        lax.fori_loop(0, DIM // QW, one, 0)

    u_copy(blk_x, 0, X_LINK, x_nbr).wait_recv()
    u_copy(blk_x, 0, RELAY, y_nbr).start()
    u_fwd(blk_x, core, X_LINK, 0).start()
    u_copy(blk_y, 1, Y_LINK, y_nbr).wait_recv()
    u_copy(blk_y, 1, RELAY, x_nbr).start()
    u_fwd(blk_y, core, Y_LINK, 1).start()

    rdma(ish.at[1 - core], ish.at[1 - core], misc_s.at[S_IN], misc_r.at[S_IN], sibling).wait_recv()
    wait_slot(4)
    for j in range(2):
        acc = jnp.dot(ish[0], ring[4, j * HALF:j * HALF + QW, :], preferred_element_type=F32)
        acc = acc + jnp.dot(ish[1], ring[4, j * HALF + QW:(j + 1) * HALF, :], preferred_element_type=F32)
        base[:, j * QW:(j + 1) * QW] = mbuf[core, :, j * QW:(j + 1) * QW].astype(F32) + acc.astype(BF16).astype(F32)
    start_gu_block(24)
    dispatch(blk0, 0)
    rdma(ids_all.at[1 - dy], ids_all.at[1 - dy], misc_s.at[S_IDS], misc_r.at[S_IDS], y_nbr).wait_recv()
    rdma(gates_all.at[1 - dy], gates_all.at[1 - dy], misc_s.at[S_GATES], misc_r.at[S_GATES], y_nbr).wait_recv()
    u_copy(blk_x, 1, X_LINK, x_nbr).wait_recv()
    u_fwd(blk_x, core, X_LINK, 1).start()
    u_copy(blk_y, 0, Y_LINK, y_nbr).wait_recv()
    u_fwd(blk_y, core, Y_LINK, 0).start()
    for xb in range(2):
        route_block(1 - dy, xb)
    for h in range(2):
        u_fwd(blk_x, 1 - core, X_LINK, h).wait_recv()
    dispatch(blk_x, 0)
    u_copy(blk_d, 0, RELAY, y_nbr).wait_recv()
    u_fwd(blk_d, core, RELAY, 0).start()
    u_copy(blk_d, 1, RELAY, x_nbr).wait_recv()
    u_fwd(blk_d, core, RELAY, 1).start()
    for h in range(2):
        u_fwd(blk_y, 1 - core, Y_LINK, h).wait_recv()
    dispatch(blk_y, 0)
    for h in range(2):
        u_fwd(blk_d, 1 - core, RELAY, h).wait_recv()
    dispatch(blk_d, 0)

    def in_part(e, c):
        return inner.at[e, :, pl.ds(pl.multiple_of(c * QW, QW), QW)]

    def in_copy(e, c):
        return rdma(in_part(e, c), in_part(e, c), in_s.at[e], in_r.at[e], sibling)

    def expert_pair(p, after):
        slots = [lax.rem(5 + 4 * p + i, RING) for i in range(4)]
        for slot in slots:
            wait_slot(slot)
        for i in range(2):
            e = 2 * p + i
            rows = xe[e & (XE - 1)]
            gate = jnp.dot(rows, ring[slots[2 * i]], preferred_element_type=F32)
            up = jnp.dot(rows, ring[slots[2 * i + 1]], preferred_element_type=F32)
            inner[e, :, pl.ds(pl.multiple_of(core * QW, QW), QW)] = (jax.nn.silu(gate) * up).astype(BF16)
        for i in range(2):
            in_copy(2 * p + i, core).start()
        after(p, slots)

    def refill(p, slots):
        @pl.when(p < 3)
        def _():
            for i in range(2):
                start_gate(2 * p + i + 10, slots[2 * i])
                start_up(2 * p + i + 10, slots[2 * i + 1])

        @pl.when((p >= 3) & (p < 7))
        def _():
            for i in range(4):
                start_down(4 * (p - 3) + i, slots[i])

    lax.fori_loop(0, 4, lambda p, c: (expert_pair(p, refill), c)[1], 0)
    lax.fori_loop(0, 4, lambda b, c: (dispatch(b, 1), c)[1], 0)
    lax.fori_loop(4, 8, lambda p, c: (expert_pair(p, refill), c)[1], 0)

    top = pl.ds(0, ROWS_Y)
    low = pl.ds(ROWS_Y, ROWS - ROWS_Y)

    def stage1(k, i):
        if i == 0:
            return [rdma(pbuf.at[k, blk_d, part, :], recv1.at[k, 0, part, :], p1_s.at[k, 0, a], p1_r.at[k, 0, a], dev)
                    for a, (part, dev) in enumerate(((top, y_nbr), (low, x_nbr)))]
        return [rdma(pbuf.at[k, b, part, :], recv1.at[k, 1, part, :], p1_s.at[k, 1, a], p1_r.at[k, 1, a], dev)
                for a, (b, part, dev) in enumerate(((blk_y, top, y_nbr), (blk_x, low, x_nbr)))]

    def stage2(k):
        return [rdma(send2.at[k, part, :], recv2.at[k, part, :], p2_s.at[k, a], p2_r.at[k, a], dev)
                for a, (part, dev) in enumerate(((top, x_nbr), (low, y_nbr)))]

    def run_stage2(k):
        first, second = stage1(k, 0)
        going = stage2(k)
        first.wait_recv()
        send2[k, 0:ROWS_Y, :] = pbuf[k, blk_x, 0:ROWS_Y, :] + recv1[k, 0, 0:ROWS_Y, :]
        going[0].start()
        second.wait_recv()
        send2[k, ROWS_Y:ROWS, :] = pbuf[k, blk_y, ROWS_Y:ROWS, :] + recv1[k, 0, ROWS_Y:ROWS, :]
        going[1].start()

    def o_part(x, c, k):
        return oall.at[x, c, k]

    def store_out(x, c, k, which):
        return pltpu.make_async_copy(o_part(x, c, k),
                                     out_ref.at[pl.ds(x * ROWS, ROWS), pl.ds(pl.multiple_of(c * HALF + k * CW, CW), CW)],
                                     out_sem.at[which, k])

    def o_sib(k, c):
        return rdma(o_part(cx, c, k), o_part(cx, c, k), os_s.at[k], os_r.at[k], sibling)

    def o_x(k, x):
        return rdma(o_part(x, core, k), o_part(x, core, k), ox_s.at[k], ox_r.at[k], x_nbr)

    def o_fwd(k, c):
        return rdma(o_part(1 - cx, c, k), o_part(1 - cx, c, k), of_s.at[k], of_r.at[k], sibling)

    def run_final(k):
        for cp in stage1(k, 1):
            cp.wait_recv()
        for cp in stage2(k):
            cp.wait_recv()
        routed = pbuf[k, blk0] + recv1[k, 1] + recv2[k]
        oall[cx, core, k] = (base[:, k * CW:(k + 1) * CW] + routed).astype(BF16)
        o_x(k, cx).start()
        o_sib(k, core).start()
        store_out(cx, core, k, 0).start()

    def run_forward(k):
        o_x(k, 1 - cx).wait_recv()
        o_fwd(k, core).start()
        store_out(1 - cx, core, k, 1).start()

    for e in range(EXPERTS):
        in_copy(e, 1 - core).wait_recv()

    for k in range(CHUNKS):
        def down_group(g, carry):
            slot = lax.rem(37 + 4 * k + g, RING)
            wait_slot(slot)
            for i in range(4):
                e = g * 4 + i
                w = ring[slot, (i // 2) * HALF:(i // 2 + 1) * HALF, (i % 2) * CW:(i % 2 + 1) * CW]
                res = jnp.dot(inner[e], w, preferred_element_type=F32).astype(BF16)
                for b in range(4):
                    ybuf[b, pl.ds(pl.multiple_of(e * SLOTS, SLOTS), SLOTS), :] = res[b * SLOTS:(b + 1) * SLOTS, :]
            return carry
        lax.fori_loop(0, 4, down_group, 0)

        def combine(b):
            res = jnp.dot(cg[b], ybuf[b], preferred_element_type=F32)
            pbuf[k, b] = res[0:ROWS] + res[ROWS:256] + res[256:384]
        combine(blk_d)
        for cp in stage1(k, 0):
            cp.start()
        combine(blk_y)
        combine(blk_x)
        for cp in stage1(k, 1):
            cp.start()
        combine(blk0)
        if k >= 1:
            run_stage2(k - 1)
        if k >= 2:
            run_final(k - 2)
    run_stage2(CHUNKS - 1)
    run_final(CHUNKS - 2)
    for k in range(CHUNKS - 1):
        run_forward(k)
    run_final(CHUNKS - 1)
    run_forward(CHUNKS - 1)
    for k in range(CHUNKS):
        o_sib(k, 1 - core).wait_recv()
        store_out(cx, 1 - core, k, 2).start()
    for k in range(CHUNKS):
        o_fwd(k, 1 - core).wait_recv()
        store_out(1 - cx, 1 - core, k, 3).start()

    for cp in (ctx_cp, m_cp, ids_cp, gates_cp, ish_cp):
        cp.wait_send()
    for h in range(2):
        u_copy(blk0, h, X_LINK, x_nbr).wait_send()
        u_copy(blk0, h, Y_LINK, y_nbr).wait_send()
        u_fwd(blk_x, core, X_LINK, h).wait_send()
        u_fwd(blk_y, core, Y_LINK, h).wait_send()
        u_fwd(blk_d, core, RELAY, h).wait_send()
    u_copy(blk_x, 0, RELAY, y_nbr).wait_send()
    u_copy(blk_y, 1, RELAY, x_nbr).wait_send()
    for e in range(EXPERTS):
        in_copy(e, core).wait_send()
    for k in range(CHUNKS):
        for cp in stage1(k, 0) + stage1(k, 1) + stage2(k):
            cp.wait_send()
        o_sib(k, core).wait_send()
        o_x(k, cx).wait_send()
        o_fwd(k, core).wait_send()
        store_out(cx, core, k, 0).wait()
        store_out(1 - cx, core, k, 1).wait()
        store_out(cx, 1 - core, k, 2).wait()
        store_out(1 - cx, 1 - core, k, 3).wait()


def moe(ctx, ids, gates, gain, hidden, w_o, sg, su, sd, wg, wu, wd):
    any_spec = pl.BlockSpec(memory_space=pl.ANY)
    vmem_spec = pl.BlockSpec(memory_space=pltpu.VMEM)
    dma = pltpu.SemaphoreType.DMA
    return pl.pallas_call(
        moe_kernel,
        out_shape=jax.ShapeDtypeStruct(hidden.shape, BF16),
        in_specs=[vmem_spec] + [any_spec] * 11,
        out_specs=any_spec,
        scratch_shapes=[
            pltpu.VMEM((RING, DIM, QW), BF16),
            pltpu.VMEM((ROWS, HALF), BF16),
            pltpu.VMEM((ROWS, HALF), BF16),
            pltpu.VMEM((ROWS, HALF), BF16),
            pltpu.VMEM((2, ROWS, HALF), BF16),
            pltpu.VMEM((4, ROWS, DIM), BF16),
            pltpu.VMEM((2, ROWS, QW), BF16),
            pltpu.VMEM((ROWS, HALF), F32),
            pltpu.VMEM((2, 8, 2 * ROWS), jnp.int32),
            pltpu.VMEM((2, 8, 2 * ROWS), F32),
            pltpu.VMEM((4, EXPERTS * SLOTS, ROWS), BF16),
            pltpu.VMEM((4, 3 * ROWS, EXPERTS * SLOTS), BF16),
            pltpu.VMEM((XE, 4 * SLOTS, DIM), BF16),
            pltpu.VMEM((EXPERTS, 4 * SLOTS, HALF), BF16),
            pltpu.VMEM((4, EXPERTS * SLOTS, CW), BF16),
            pltpu.VMEM((CHUNKS, 4, ROWS, CW), F32),
            pltpu.VMEM((CHUNKS, 2, ROWS, CW), F32),
            pltpu.VMEM((CHUNKS, ROWS, CW), F32),
            pltpu.VMEM((CHUNKS, ROWS, CW), F32),
            pltpu.VMEM((2, 2, CHUNKS, ROWS, CW), BF16),
            dma((RING,)), dma((4,)), dma((5,)), dma((5,)),
            dma((3, 2)), dma((3, 2)), dma((3, 2)), dma((3, 2)),
            dma((EXPERTS,)), dma((EXPERTS,)),
            dma((CHUNKS, 2, 2)), dma((CHUNKS, 2, 2)), dma((CHUNKS, 2)), dma((CHUNKS, 2)),
            dma((CHUNKS,)), dma((CHUNKS,)), dma((CHUNKS,)), dma((CHUNKS,)), dma((CHUNKS,)), dma((CHUNKS,)),
            dma((4, CHUNKS)),
        ],
        compiler_params=pltpu.CompilerParams(vmem_limit_bytes=63 * HALF * HALF, collective_id=0, has_side_effects=True),
        name='experts',
    )(gain, ctx, ids, gates, hidden, w_o, sg, su, sd, wg, wu, wd)


def solution(mesh):
    batch_spec = P(('inst', 'dev'))
    layer_batch = P(None, ('inst', 'dev'))
    expert_spec = P(None, 'dev')

    def device_fn(hidden, k_cache, v_cache, cache_lens, expert_ids, route_gates, attn_gain, ffn_gain, w_q, w_kv, w_o, shared_gate, shared_up, shared_down, w_gate, w_up, w_down):
        ctx = attention(hidden, cache_lens, attn_gain, w_q, w_kv, k_cache, v_cache)
        return moe(ctx, expert_ids[0].T, route_gates[0].T, ffn_gain, hidden, w_o, shared_gate, shared_up, shared_down, w_gate, w_up, w_down)

    in_specs = (batch_spec, layer_batch, layer_batch, batch_spec, layer_batch, layer_batch, P(), P(), P(), P(), P(), P(), P(), P(), expert_spec, expert_spec, expert_spec)
    return jax.shard_map(device_fn, mesh=mesh, in_specs=in_specs, out_specs=batch_spec, check_vma=False)
```

```python
import functools

import numpy as np
import jax
import jax.numpy as jnp
from jax import lax
from jax.experimental import pallas as pl
from jax.experimental.pallas import tpu as pltpu
from jax.sharding import PartitionSpec as P

NORM_EPS = 1e-6
ROPE_BASE = 10000.0
MESH = pl.DeviceIdType.MESH
LAST_DIMS = (((1,), (1,)), ((), ()))
F32 = jnp.float32
BF16 = jnp.bfloat16

ROWS = 128
HEADS = 8
HD = 128
DIM = 2048
HALF = DIM // 2
HH = HEADS // 2
GROUP = 8
KV_RING = 8
PAIRS = ROWS // (2 * GROUP)
RING = 20
QW = 512
LAYER = 0
S_CTX, S_IDS, S_M, S_IN, S_GATES = range(5)
X_LINK, Y_LINK, RELAY = range(3)
XE = 8
EXPERTS = 16
SLOTS = 32
CHUNKS = 4
CW = HALF // CHUNKS
ROWS_Y = (72, 104, 72, 64)


def norm_rows(rows_f, gain):
    inv_rms = lax.rsqrt(jnp.mean(rows_f * rows_f, axis=-1, keepdims=True) + NORM_EPS)
    return (rows_f * inv_rms * gain).astype(BF16)


def attn_kernel(lens_ref, hidden_ref, gain_ref, freq_ref, wq_ref, wkv_ref, kc_ref, vc_ref, ctx_ref,
                xbuf, nbuf, cosbuf, sinbuf, wbuf, pos_buf, qbuf, nkbuf, nvbuf, cbuf, sbuf, pbuf, kbuf, vbuf, xsem, wsem, ksem, vsem):
    side = lax.axis_index('side')
    row0 = (side // 2) * ROWS
    core = side % 2
    h0 = core * HEADS

    def size_of(tok):
        return (lens_ref[row0 + tok] + 15) & -16

    def first_token(unit, d):
        return (unit & (PAIRS - 1)) * (2 * GROUP) + d * GROUP

    def start_unit(unit):
        slot = unit & (KV_RING - 1)
        heads = pl.ds(h0 + (unit >> 3) * HH, HH)
        for d in range(2):
            for i in range(GROUP):
                tok = first_token(unit, d) + i
                size = pl.multiple_of(size_of(tok), 16)
                for src, dst, sem in ((kc_ref, kbuf, ksem), (vc_ref, vbuf, vsem)):
                    pltpu.make_async_copy(src.at[LAYER, row0 + tok, heads, pl.ds(0, size), :],
                                          dst.at[slot, pl.ds(d * HH, HH), pl.ds(i * HD, size), :], sem.at[slot, d]).start()

    def wait_unit(unit, buf, sem):
        slot = unit & (KV_RING - 1)
        for d in range(2):
            total = sum(size_of(first_token(unit, d) + i) for i in range(GROUP))
            whole = buf.at[slot, pl.ds(d * HH, HH), pl.ds(0, pl.multiple_of(total, 16)), :]
            pltpu.make_async_copy(whole, whole, sem.at[slot, d]).wait()

    x_cp = pltpu.make_async_copy(hidden_ref.at[pl.ds(row0, ROWS), :], xbuf, xsem)
    x_cp.start()

    def weight_copy(j, kind):
        col = core * HALF + j * QW
        if kind == 0:
            src = wq_ref.at[LAYER, :, pl.ds(col, QW)]
        else:
            src = wkv_ref.at[LAYER, :, pl.ds((kind - 1) * DIM + col, QW)]
        return pltpu.make_async_copy(src, wbuf.at[j * 3 + kind], wsem.at[j * 3 + kind])

    def start_units(lo, hi):
        def one(unit, carry):
            for h in range(2 * HH):
                vbuf[unit, h] = jnp.zeros((GROUP * HD, HD), BF16)
            start_unit(unit)
            return carry
        lax.fori_loop(lo, hi, one, 0)
    for kind in range(3):
        weight_copy(0, kind).start()

    def fill_pos(i, carry):
        for r in range(8):
            row = i * 8 + r
            pos_buf[pl.ds(row, 1), :] = jnp.full((1, HD), lens_ref[row0 + row].astype(F32), F32)
        return carry
    lax.fori_loop(0, ROWS // 8, fill_pos, 0)
    angles = pos_buf[...] * freq_ref[...]
    cosine = jnp.cos(angles)
    lane = lax.broadcasted_iota(jnp.int32, (ROWS, HD), 1)
    sine = jnp.sin(angles)
    sine = jnp.where(lane < HD // 2, -sine, sine)

    start_units(0, 2)
    for kind in range(3):
        weight_copy(1, kind).start()
    x_cp.wait()
    nbuf[...] = norm_rows(xbuf[...].astype(F32), gain_ref[...])
    cosbuf[...] = cosine
    sinbuf[...] = sine
    start_units(2, KV_RING)

    def project(j):
        for kind in range(3):
            weight_copy(j, kind).wait()
            res = jnp.dot(nbuf[...], wbuf[j * 3 + kind], preferred_element_type=F32).astype(BF16).astype(F32)
            for hh in range(HH):
                h = j * HH + hh
                val = res[:, hh * HD:(hh + 1) * HD]
                if kind < 2:
                    val = (val * cosbuf[...] + pltpu.roll(val, HD // 2, 1) * sinbuf[...]).astype(BF16).astype(F32)
                (qbuf, nkbuf, nvbuf)[kind][:, h * HD:(h + 1) * HD] = val
    project(0)

    row_id = lax.broadcasted_iota(jnp.int32, (2 * GROUP, HD), 0) & (GROUP - 1)
    lane_f = lax.broadcasted_iota(jnp.int32, (GROUP, HD), 1).astype(F32)

    def parts_of(unit):
        for d in range(2):
            rows = pl.ds(pl.multiple_of(first_token(unit, d), GROUP), GROUP)
            for hp in range(2):
                head = (unit >> 3) * HH + 2 * hp
                cols = [pl.ds(pl.multiple_of((head + p) * HD, HD), HD) for p in range(2)]
                yield 2 * d + hp, d * HH + 2 * hp, rows, cols

    def score_unit(unit):
        slot = unit & (KV_RING - 1)
        zero = jnp.zeros((GROUP, HD), F32)
        for n, at, rows, cols in parts_of(unit):
            valid = lane_f < pos_buf[rows, :]
            valid = jnp.concatenate([valid, valid], axis=0)
            first = jnp.concatenate([qbuf[rows, cols[0]], zero], axis=0)
            second = jnp.concatenate([zero, qbuf[rows, cols[1]]], axis=0)
            lhs = jnp.concatenate([first, second], axis=1).astype(BF16)
            rhs = jnp.concatenate([kbuf[slot, at], kbuf[slot, at + 1]], axis=1)
            full = lax.dot_general(lhs, rhs, LAST_DIMS, preferred_element_type=F32)
            sc = full[:, 0:HD]
            for i in range(1, GROUP):
                sc = jnp.where(row_id == i, full[:, i * HD:(i + 1) * HD], sc)
            sbuf[unit & 1, n] = jnp.where(valid, sc * (HD ** -0.5), -jnp.inf)

    def soften_unit(unit):
        for n, at, rows, cols in parts_of(unit):
            sc = sbuf[unit & 1, n]
            q_k = [jnp.concatenate([ref[rows, c] for c in cols], axis=0) for ref in (qbuf, nkbuf)]
            self_sc = jnp.sum(q_k[0] * q_k[1], axis=-1, keepdims=True) * (HD ** -0.5)
            peak = jnp.maximum(jnp.max(sc, axis=-1, keepdims=True), self_sc)
            wts = jnp.exp(sc - peak)
            self_w = jnp.exp(self_sc - peak)
            denom = jnp.sum(wts, axis=-1, keepdims=True) + self_w
            prob = wts / denom
            self_p = (self_w / denom).astype(BF16).astype(F32)
            wide = jnp.concatenate([jnp.where(row_id == i, prob, 0.0) for i in range(GROUP)], axis=1).astype(BF16)
            pbuf[unit & 1, n] = wide
            for p in range(2):
                cbuf[rows, cols[p]] = self_p[p * GROUP:(p + 1) * GROUP] * nvbuf[rows, cols[p]]

    def value_unit(unit):
        slot = unit & (KV_RING - 1)
        for n, at, rows, cols in parts_of(unit):
            rhs = jnp.concatenate([vbuf[slot, at], vbuf[slot, at + 1]], axis=1)
            ctx = jnp.dot(pbuf[unit & 1, n], rhs, preferred_element_type=F32)
            for p in range(2):
                cbuf[rows, cols[p]] += ctx[p * GROUP:(p + 1) * GROUP, p * HD:(p + 1) * HD]

    last = 2 * PAIRS - 1
    wait_unit(jnp.int32(0), kbuf, ksem)
    score_unit(jnp.int32(0))
    wait_unit(jnp.int32(1), kbuf, ksem)
    soften_unit(jnp.int32(0))
    score_unit(jnp.int32(1))

    def body(unit, carry):
        wait_unit(unit - 1, vbuf, vsem)
        wait_unit(unit + 1, kbuf, ksem)
        value_unit(unit - 1)
        soften_unit(unit)
        score_unit(unit + 1)

        @pl.when(unit - 1 + KV_RING <= last)
        def _():
            start_unit(unit - 1 + KV_RING)
        return carry
    lax.fori_loop(1, PAIRS - 1, body, 0)
    project(1)
    lax.fori_loop(PAIRS - 1, last, body, 0)
    wait_unit(jnp.int32(last - 1), vbuf, vsem)
    wait_unit(jnp.int32(last), vbuf, vsem)
    value_unit(jnp.int32(last - 1))
    soften_unit(jnp.int32(last))
    value_unit(jnp.int32(last))
    ctx_ref[...] = cbuf[...].astype(BF16)


def attention(hidden, lens, gain, w_q, w_kv, k_cache, v_cache):
    freq = ROPE_BASE ** (-np.arange(HD // 2, dtype=np.float64) * 2.0 / HD)
    freq = np.concatenate([freq, freq])[None, :].astype(np.float32)
    any_spec = pl.BlockSpec(memory_space=pl.ANY)
    vmem_spec = pl.BlockSpec(memory_space=pltpu.VMEM)
    return pl.pallas_call(
        attn_kernel,
        out_shape=jax.ShapeDtypeStruct((ROWS, HALF), BF16),
        in_specs=[pl.BlockSpec(memory_space=pltpu.SMEM), any_spec, vmem_spec, vmem_spec] + [any_spec] * 4,
        out_specs=vmem_spec,
        scratch_shapes=[
            pltpu.VMEM((ROWS, DIM), BF16),
            pltpu.VMEM((ROWS, DIM), BF16),
            pltpu.VMEM((ROWS, HD), F32),
            pltpu.VMEM((ROWS, HD), F32),
            pltpu.VMEM((6, DIM, QW), BF16),
            pltpu.VMEM((ROWS, HD), F32),
            pltpu.VMEM((ROWS, HALF), F32),
            pltpu.VMEM((ROWS, HALF), F32),
            pltpu.VMEM((ROWS, HALF), F32),
            pltpu.VMEM((ROWS, HALF), F32),
            pltpu.VMEM((2, HEADS // 2, 2 * GROUP, HD), F32),
            pltpu.VMEM((2, HEADS // 2, 2 * GROUP, GROUP * HD), BF16),
            pltpu.VMEM((KV_RING, 2 * HH, GROUP * HD, HD), BF16),
            pltpu.VMEM((KV_RING, 2 * HH, GROUP * HD, HD), BF16),
            pltpu.SemaphoreType.DMA,
            pltpu.SemaphoreType.DMA((6,)),
            pltpu.SemaphoreType.DMA((KV_RING, 2)),
            pltpu.SemaphoreType.DMA((KV_RING, 2)),
        ],
        compiler_params=pltpu.CompilerParams(vmem_limit_bytes=60 * HALF * HALF),
        name='attend',
    )(lens, hidden, gain, jnp.asarray(freq), w_q, w_kv, k_cache, v_cache)


def moe_kernel(gain_ref, ctx_ref, ids_ref, gates_ref, hidden_ref, wo_ref, sg_ref, su_ref, sd_ref, wg_ref, wu_ref, wd_ref, out_ref,
               ring, ctx_own, ctx_sib, xbuf, mbuf, uall, ish, base, ids_all, gates_all, dmat, cg, xe, inner, ybuf, pbuf,
               recv1, send2, recv2, oall,
               ring_sem, x_sem, misc_s, misc_r, u_s, u_r, uf_s, uf_r, in_s, in_r, p1_s, p1_r, p2_s, p2_r,
               os_s, os_r, ox_s, ox_r, of_s, of_r, out_sem):
    inst = lax.axis_index('inst')
    dy = lax.axis_index('dev')
    side = lax.axis_index('side')
    cx = side // 2
    core = side % 2
    blk0 = dy * 2 + cx
    col0 = core * HALF

    def dev_of(y, x, c):
        return (inst, y, x * 2 + c)
    sibling = dev_of(dy, cx, 1 - core)
    x_nbr = dev_of(dy, 1 - cx, core)
    y_nbr = dev_of(1 - dy, cx, core)

    def rdma(src, dst, s_sem, r_sem, dev):
        return pltpu.make_async_remote_copy(src_ref=src, dst_ref=dst, send_sem=s_sem, recv_sem=r_sem,
                                            device_id=dev, device_id_type=MESH)

    def start_wo(j):
        pltpu.make_async_copy(wo_ref.at[LAYER, :, pl.ds(col0 + j * QW, QW)], ring.at[j], ring_sem.at[j]).start()

    def start_gate(e, slot):
        pltpu.make_async_copy(wg_ref.at[LAYER, cx * EXPERTS + e, :, pl.ds(core * QW, QW)], ring.at[slot], ring_sem.at[slot]).start()

    def start_up(e, slot):
        pltpu.make_async_copy(wu_ref.at[LAYER, cx * EXPERTS + e, :, pl.ds(core * QW, QW)], ring.at[slot], ring_sem.at[slot]).start()

    def start_down(m, slot):
        k = m >> 2
        g = m & 3
        for i in range(4):
            pltpu.make_async_copy(wd_ref.at[LAYER, cx * EXPERTS + g * 4 + i, :, pl.ds(col0 + k * CW, CW)],
                                  ring.at[slot, pl.ds((i // 2) * HALF, HALF), pl.ds((i % 2) * CW, CW)],
                                  ring_sem.at[slot]).start()

    def wait_slot(slot):
        pltpu.make_async_copy(wg_ref.at[LAYER, 0, :, pl.ds(0, QW)], ring.at[slot], ring_sem.at[slot]).wait()

    def start_gu_block(b):
        e, up = (b - 5) // 2, (b - 5) % 2
        (start_up if up else start_gate)(e, b % RING)

    ctx_in = pltpu.make_async_copy(ctx_ref, ctx_own, x_sem.at[0])
    ctx_in.start()
    start_wo(0)
    start_wo(1)
    x_cp = pltpu.make_async_copy(hidden_ref.at[pl.ds(cx * ROWS, ROWS), pl.ds(col0, HALF)], xbuf, x_sem.at[1])
    x_cp.start()

    barrier = pltpu.get_barrier_semaphore()
    for dev in (sibling, x_nbr, y_nbr):
        pl.semaphore_signal(barrier, inc=1, device_id=dev, device_id_type=MESH)
    pltpu.make_async_copy(sg_ref.at[LAYER, :, pl.ds(core * QW, QW)], ring.at[2], ring_sem.at[2]).start()
    pltpu.make_async_copy(su_ref.at[LAYER, :, pl.ds(core * QW, QW)], ring.at[3], ring_sem.at[3]).start()
    ids_in = pltpu.make_async_copy(ids_ref, ids_all.at[dy], x_sem.at[2])
    gates_in = pltpu.make_async_copy(gates_ref, gates_all.at[dy], x_sem.at[3])
    ids_in.start()
    gates_in.start()
    pl.semaphore_wait(barrier, 3)

    ctx_in.wait()
    ctx_cp = rdma(ctx_own, ctx_sib, misc_s.at[S_CTX], misc_r.at[S_CTX], sibling)
    ctx_cp.start()

    own_row = core * HALF
    sib_row = (1 - core) * HALF
    wait_slot(0)
    wait_slot(1)
    for j in range(2):
        pltpu.make_async_copy(sd_ref.at[LAYER, :, pl.ds(col0 + j * QW, QW)], ring.at[4, pl.ds(j * HALF, HALF), :],
                              ring_sem.at[4]).start()
    for b in range(5, 9):
        start_gu_block(b)
    x_cp.wait()
    ctx_val = ctx_own[...]
    accs = [jnp.dot(ctx_val, ring[j, pl.ds(own_row, HALF), :], preferred_element_type=F32) for j in range(2)]
    ctx_cp.wait_recv()
    ctx_val = ctx_sib[...]
    for j in range(2):
        acc = accs[j] + jnp.dot(ctx_val, ring[j, pl.ds(sib_row, HALF), :], preferred_element_type=F32)
        mbuf[core, :, j * QW:(j + 1) * QW] = (xbuf[:, j * QW:(j + 1) * QW].astype(F32) + acc).astype(BF16)
    m_cp = rdma(mbuf.at[core], mbuf.at[core], misc_s.at[S_M], misc_r.at[S_M], sibling)
    m_cp.start()
    for b in range(9, 22):
        start_gu_block(b)
    m_other = rdma(mbuf.at[1 - core], mbuf.at[1 - core], misc_s.at[S_M], misc_r.at[S_M], sibling)
    m_other.wait_recv()
    m_lo = mbuf[0].astype(F32)
    m_hi = mbuf[1].astype(F32)
    total = jnp.sum(m_lo * m_lo, axis=-1, keepdims=True) + jnp.sum(m_hi * m_hi, axis=-1, keepdims=True)
    inv_rms = lax.rsqrt(total / DIM + NORM_EPS)
    uall[blk0, :, 0:HALF] = (m_lo * inv_rms * gain_ref[:, 0:HALF]).astype(BF16)
    uall[blk0, :, HALF:DIM] = (m_hi * inv_rms * gain_ref[:, HALF:DIM]).astype(BF16)

    blk_x = dy * 2 + 1 - cx
    blk_y = (1 - dy) * 2 + cx
    blk_d = (1 - dy) * 2 + 1 - cx

    def u_part(b, c, h):
        return uall.at[b, pl.ds(c * 64 + h * 32, 32), :]

    def u_copy(b, h, which, dev):
        return rdma(u_part(b, core, h), u_part(b, core, h), u_s.at[which, h], u_r.at[which, h], dev)

    def u_fwd(b, c, which, h):
        return rdma(u_part(b, c, h), u_part(b, c, h), uf_s.at[which, h], uf_r.at[which, h], sibling)
    u_copy(blk0, 0, X_LINK, x_nbr).start()
    u_copy(blk0, 1, Y_LINK, y_nbr).start()
    u_copy(blk0, 1, X_LINK, x_nbr).start()
    u_copy(blk0, 0, Y_LINK, y_nbr).start()
    ids_in.wait()
    gates_in.wait()
    ids_cp = rdma(ids_all.at[dy], ids_all.at[dy], misc_s.at[S_IDS], misc_r.at[S_IDS], y_nbr)
    gates_cp = rdma(gates_all.at[dy], gates_all.at[dy], misc_s.at[S_GATES], misc_r.at[S_GATES], y_nbr)
    ids_cp.start()
    gates_cp.start()

    wait_slot(2)
    wait_slot(3)
    u_own = uall[blk0]
    gate = jnp.dot(u_own, ring[2], preferred_element_type=F32)
    up = jnp.dot(u_own, ring[3], preferred_element_type=F32)
    ish[core] = (jax.nn.silu(gate) * up).astype(BF16)
    ish_cp = rdma(ish.at[core], ish.at[core], misc_s.at[S_IN], misc_r.at[S_IN], sibling)
    ish_cp.start()
    start_gu_block(22)
    start_gu_block(23)

    expert_id = dy * 32 + cx * EXPERTS + lax.broadcasted_iota(jnp.int32, (EXPERTS, ROWS), 0)
    before = (lax.broadcasted_iota(jnp.int32, (ROWS, ROWS), 0) < lax.broadcasted_iota(jnp.int32, (ROWS, ROWS), 1))
    before = jnp.where(before, 1.0, 0.0).astype(BF16)
    slot_id = lax.broadcasted_iota(jnp.int32, (SLOTS, ROWS), 0).astype(F32)

    def route_block(yb, xb):
        b = yb * 2 + xb
        hit = jnp.zeros((EXPERTS, ROWS), F32)
        wts = jnp.zeros((EXPERTS, ROWS), F32)
        for j in range(8):
            same = ids_all[yb, j:j + 1, xb * ROWS:(xb + 1) * ROWS] == expert_id
            hit = jnp.where(same, 1.0, hit)
            wts = jnp.where(same, gates_all[yb, j:j + 1, xb * ROWS:(xb + 1) * ROWS], wts)
        place = jnp.dot(hit.astype(BF16), before, preferred_element_type=F32)
        place = jnp.where(hit > 0.5, place, -1.0)
        pieces = []
        for e in range(EXPERTS):
            match = place[e:e + 1, :] == slot_id
            dmat[b, e * SLOTS:(e + 1) * SLOTS, :] = jnp.where(match, 1.0, 0.0).astype(BF16)
            pieces.append(jnp.where(match, wts[e:e + 1, :], 0.0))
        for q in range(4):
            part = jnp.concatenate(pieces[q * 4:(q + 1) * 4], axis=0).T
            high = part.astype(BF16)
            rest = part - high.astype(F32)
            mid = rest.astype(BF16)
            low = (rest - mid.astype(F32)).astype(BF16)
            cg[b, 0:ROWS, q * ROWS:(q + 1) * ROWS] = high
            cg[b, ROWS:256, q * ROWS:(q + 1) * ROWS] = mid
            cg[b, 256:384, q * ROWS:(q + 1) * ROWS] = low

    for xb in range(2):
        route_block(dy, xb)

    half_rows = XE * SLOTS

    def dispatch(b, part):
        def one(n, carry):
            cols = pl.ds(pl.multiple_of(n * QW, QW), QW)
            rows = jnp.dot(dmat[b, part * half_rows:(part + 1) * half_rows, :], uall[b, :, cols],
                           preferred_element_type=F32).astype(BF16)
            for e in range(XE):
                xe[e, pl.ds(pl.multiple_of(b * SLOTS, SLOTS), SLOTS), cols] = rows[e * SLOTS:(e + 1) * SLOTS, :]
            return carry
        lax.fori_loop(0, DIM // QW, one, 0)

    u_copy(blk_x, 0, X_LINK, x_nbr).wait_recv()
    u_copy(blk_x, 0, RELAY, y_nbr).start()
    u_fwd(blk_x, core, X_LINK, 0).start()
    u_copy(blk_y, 1, Y_LINK, y_nbr).wait_recv()
    u_copy(blk_y, 1, RELAY, x_nbr).start()
    u_fwd(blk_y, core, Y_LINK, 1).start()

    rdma(ish.at[1 - core], ish.at[1 - core], misc_s.at[S_IN], misc_r.at[S_IN], sibling).wait_recv()
    wait_slot(4)
    for j in range(2):
        acc = jnp.dot(ish[0], ring[4, j * HALF:j * HALF + QW, :], preferred_element_type=F32)
        acc = acc + jnp.dot(ish[1], ring[4, j * HALF + QW:(j + 1) * HALF, :], preferred_element_type=F32)
        base[:, j * QW:(j + 1) * QW] = mbuf[core, :, j * QW:(j + 1) * QW].astype(F32) + acc.astype(BF16).astype(F32)
    start_gu_block(24)
    dispatch(blk0, 0)
    rdma(ids_all.at[1 - dy], ids_all.at[1 - dy], misc_s.at[S_IDS], misc_r.at[S_IDS], y_nbr).wait_recv()
    rdma(gates_all.at[1 - dy], gates_all.at[1 - dy], misc_s.at[S_GATES], misc_r.at[S_GATES], y_nbr).wait_recv()
    u_copy(blk_x, 1, X_LINK, x_nbr).wait_recv()
    u_fwd(blk_x, core, X_LINK, 1).start()
    u_copy(blk_y, 0, Y_LINK, y_nbr).wait_recv()
    u_fwd(blk_y, core, Y_LINK, 0).start()
    for xb in range(2):
        route_block(1 - dy, xb)
    for h in range(2):
        u_fwd(blk_x, 1 - core, X_LINK, h).wait_recv()
    dispatch(blk_x, 0)
    u_copy(blk_d, 0, RELAY, y_nbr).wait_recv()
    u_fwd(blk_d, core, RELAY, 0).start()
    u_copy(blk_d, 1, RELAY, x_nbr).wait_recv()
    u_fwd(blk_d, core, RELAY, 1).start()
    for h in range(2):
        u_fwd(blk_y, 1 - core, Y_LINK, h).wait_recv()
    dispatch(blk_y, 0)
    for h in range(2):
        u_fwd(blk_d, 1 - core, RELAY, h).wait_recv()
    dispatch(blk_d, 0)

    def in_part(e, c):
        return inner.at[e, :, pl.ds(pl.multiple_of(c * QW, QW), QW)]

    def in_copy(e, c):
        return rdma(in_part(e, c), in_part(e, c), in_s.at[e], in_r.at[e], sibling)

    def expert_pair(p, after):
        slots = [lax.rem(5 + 4 * p + i, RING) for i in range(4)]
        for slot in slots:
            wait_slot(slot)
        for i in range(2):
            e = 2 * p + i
            rows = xe[e & (XE - 1)]
            gate = jnp.dot(rows, ring[slots[2 * i]], preferred_element_type=F32)
            up = jnp.dot(rows, ring[slots[2 * i + 1]], preferred_element_type=F32)
            inner[e, :, pl.ds(pl.multiple_of(core * QW, QW), QW)] = (jax.nn.silu(gate) * up).astype(BF16)
        for i in range(2):
            in_copy(2 * p + i, core).start()
        after(p, slots)

    def refill(p, slots):
        @pl.when(p < 3)
        def _():
            for i in range(2):
                start_gate(2 * p + i + 10, slots[2 * i])
                start_up(2 * p + i + 10, slots[2 * i + 1])

        @pl.when((p >= 3) & (p < 7))
        def _():
            for i in range(4):
                start_down(4 * (p - 3) + i, slots[i])

    lax.fori_loop(0, 4, lambda p, c: (expert_pair(p, refill), c)[1], 0)
    lax.fori_loop(0, 4, lambda b, c: (dispatch(b, 1), c)[1], 0)
    lax.fori_loop(4, 8, lambda p, c: (expert_pair(p, refill), c)[1], 0)

    def split(k):
        return pl.ds(0, ROWS_Y[k]), pl.ds(ROWS_Y[k], ROWS - ROWS_Y[k])

    def stage1(k, i):
        top, low = split(k)
        if i == 0:
            return [rdma(pbuf.at[k, blk_d, part, :], recv1.at[k, 0, part, :], p1_s.at[k, 0, a], p1_r.at[k, 0, a], dev)
                    for a, (part, dev) in enumerate(((top, y_nbr), (low, x_nbr)))]
        return [rdma(pbuf.at[k, b, part, :], recv1.at[k, 1, part, :], p1_s.at[k, 1, a], p1_r.at[k, 1, a], dev)
                for a, (b, part, dev) in enumerate(((blk_y, top, y_nbr), (blk_x, low, x_nbr)))]

    def stage2(k):
        return [rdma(send2.at[k, part, :], recv2.at[k, part, :], p2_s.at[k, a], p2_r.at[k, a], dev)
                for a, (part, dev) in enumerate(zip(split(k), (x_nbr, y_nbr)))]

    def run_stage2(k):
        first, second = stage1(k, 0)
        going = stage2(k)
        first.wait_recv()
        n = ROWS_Y[k]
        send2[k, 0:n, :] = pbuf[k, blk_x, 0:n, :] + recv1[k, 0, 0:n, :]
        going[0].start()
        second.wait_recv()
        send2[k, n:ROWS, :] = pbuf[k, blk_y, n:ROWS, :] + recv1[k, 0, n:ROWS, :]
        going[1].start()

    def o_part(x, c, k):
        return oall.at[x, c, k]

    def store_out(x, c, k, which):
        return pltpu.make_async_copy(o_part(x, c, k), out_part(x, c, k), out_sem.at[which, k])

    def out_part(x, c, k):
        return out_ref.at[pl.ds(x * ROWS, ROWS), pl.ds(pl.multiple_of(c * HALF + k * CW, CW), CW)]

    def o_sib(k, c):
        return rdma(o_part(cx, c, k), out_part(cx, c, k), os_s.at[k], os_r.at[k], sibling)

    def o_x(k, x):
        return rdma(o_part(x, core, k), o_part(x, core, k), ox_s.at[k], ox_r.at[k], x_nbr)

    def o_fwd(k, c):
        return rdma(o_part(1 - cx, c, k), out_part(1 - cx, c, k), of_s.at[k], of_r.at[k], sibling)

    def run_final(k):
        for cp in stage1(k, 1):
            cp.wait_recv()
        for cp in stage2(k):
            cp.wait_recv()
        routed = pbuf[k, blk0] + recv1[k, 1] + recv2[k]
        oall[cx, core, k] = (base[:, k * CW:(k + 1) * CW] + routed).astype(BF16)
        o_x(k, cx).start()
        o_sib(k, core).start()
        store_out(cx, core, k, 0).start()

    def run_forward(k):
        o_x(k, 1 - cx).wait_recv()
        o_fwd(k, core).start()
        store_out(1 - cx, core, k, 1).start()

    for k in range(CHUNKS):
        def down_group(g, carry):
            slot = lax.rem(37 + 4 * k + g, RING)
            wait_slot(slot)
            if k == 0:
                for i in range(4):
                    in_copy(g * 4 + i, 1 - core).wait_recv()
            for i in range(4):
                e = g * 4 + i
                w = ring[slot, (i // 2) * HALF:(i // 2 + 1) * HALF, (i % 2) * CW:(i % 2 + 1) * CW]
                res = jnp.dot(inner[e], w, preferred_element_type=F32).astype(BF16)
                for b in range(4):
                    ybuf[b, pl.ds(pl.multiple_of(e * SLOTS, SLOTS), SLOTS), :] = res[b * SLOTS:(b + 1) * SLOTS, :]
            return carry
        lax.fori_loop(0, 4, down_group, 0)

        def combine(b):
            res = jnp.dot(cg[b], ybuf[b], preferred_element_type=F32)
            pbuf[k, b] = res[0:ROWS] + res[ROWS:256] + res[256:384]
        combine(blk_d)
        for cp in stage1(k, 0):
            cp.start()
        combine(blk_y)
        combine(blk_x)
        for cp in stage1(k, 1):
            cp.start()
        combine(blk0)
        if k >= 1:
            run_stage2(k - 1)
    run_final(0)
    run_stage2(CHUNKS - 1)
    for k in range(1, CHUNKS):
        run_final(k)
        run_forward(k - 1)
    run_forward(CHUNKS - 1)
    for k in range(CHUNKS):
        o_sib(k, 1 - core).wait_recv()
    for k in range(CHUNKS):
        o_fwd(k, 1 - core).wait_recv()

    for cp in (ctx_cp, m_cp, ids_cp, gates_cp, ish_cp):
        cp.wait_send()
    for h in range(2):
        u_copy(blk0, h, X_LINK, x_nbr).wait_send()
        u_copy(blk0, h, Y_LINK, y_nbr).wait_send()
        u_fwd(blk_x, core, X_LINK, h).wait_send()
        u_fwd(blk_y, core, Y_LINK, h).wait_send()
        u_fwd(blk_d, core, RELAY, h).wait_send()
    u_copy(blk_x, 0, RELAY, y_nbr).wait_send()
    u_copy(blk_y, 1, RELAY, x_nbr).wait_send()
    for e in range(EXPERTS):
        in_copy(e, core).wait_send()
    for k in range(CHUNKS):
        for cp in stage1(k, 0) + stage1(k, 1) + stage2(k):
            cp.wait_send()
        o_sib(k, core).wait_send()
        o_x(k, cx).wait_send()
        o_fwd(k, core).wait_send()
        store_out(cx, core, k, 0).wait()
        store_out(1 - cx, core, k, 1).wait()


def moe(ctx, ids, gates, gain, hidden, w_o, sg, su, sd, wg, wu, wd):
    any_spec = pl.BlockSpec(memory_space=pl.ANY)
    vmem_spec = pl.BlockSpec(memory_space=pltpu.VMEM)
    dma = pltpu.SemaphoreType.DMA
    return pl.pallas_call(
        moe_kernel,
        out_shape=jax.ShapeDtypeStruct(hidden.shape, BF16),
        in_specs=[vmem_spec] + [any_spec] * 11,
        out_specs=any_spec,
        scratch_shapes=[
            pltpu.VMEM((RING, DIM, QW), BF16),
            pltpu.VMEM((ROWS, HALF), BF16),
            pltpu.VMEM((ROWS, HALF), BF16),
            pltpu.VMEM((ROWS, HALF), BF16),
            pltpu.VMEM((2, ROWS, HALF), BF16),
            pltpu.VMEM((4, ROWS, DIM), BF16),
            pltpu.VMEM((2, ROWS, QW), BF16),
            pltpu.VMEM((ROWS, HALF), F32),
            pltpu.VMEM((2, 8, 2 * ROWS), jnp.int32),
            pltpu.VMEM((2, 8, 2 * ROWS), F32),
            pltpu.VMEM((4, EXPERTS * SLOTS, ROWS), BF16),
            pltpu.VMEM((4, 3 * ROWS, EXPERTS * SLOTS), BF16),
            pltpu.VMEM((XE, 4 * SLOTS, DIM), BF16),
            pltpu.VMEM((EXPERTS, 4 * SLOTS, HALF), BF16),
            pltpu.VMEM((4, EXPERTS * SLOTS, CW), BF16),
            pltpu.VMEM((CHUNKS, 4, ROWS, CW), F32),
            pltpu.VMEM((CHUNKS, 2, ROWS, CW), F32),
            pltpu.VMEM((CHUNKS, ROWS, CW), F32),
            pltpu.VMEM((CHUNKS, ROWS, CW), F32),
            pltpu.VMEM((2, 2, CHUNKS, ROWS, CW), BF16),
            dma((RING,)), dma((4,)), dma((5,)), dma((5,)),
            dma((3, 2)), dma((3, 2)), dma((3, 2)), dma((3, 2)),
            dma((EXPERTS,)), dma((EXPERTS,)),
            dma((CHUNKS, 2, 2)), dma((CHUNKS, 2, 2)), dma((CHUNKS, 2)), dma((CHUNKS, 2)),
            dma((CHUNKS,)), dma((CHUNKS,)), dma((CHUNKS,)), dma((CHUNKS,)), dma((CHUNKS,)), dma((CHUNKS,)),
            dma((2, CHUNKS)),
        ],
        compiler_params=pltpu.CompilerParams(vmem_limit_bytes=63 * HALF * HALF, collective_id=0, has_side_effects=True),
        name='experts',
    )(gain, ctx, ids, gates, hidden, w_o, sg, su, sd, wg, wu, wd)


def solution(mesh):
    batch_spec = P(('inst', 'dev'))
    layer_batch = P(None, ('inst', 'dev'))
    expert_spec = P(None, 'dev')

    def device_fn(hidden, k_cache, v_cache, cache_lens, expert_ids, route_gates, attn_gain, ffn_gain, w_q, w_kv, w_o, shared_gate, shared_up, shared_down, w_gate, w_up, w_down):
        ctx = attention(hidden, cache_lens, attn_gain, w_q, w_kv, k_cache, v_cache)
        return moe(ctx, expert_ids[0].T, route_gates[0].T, ffn_gain, hidden, w_o, shared_gate, shared_up, shared_down, w_gate, w_up, w_down)

    in_specs = (batch_spec, layer_batch, layer_batch, batch_spec, layer_batch, layer_batch, P(), P(), P(), P(), P(), P(), P(), P(), expert_spec, expert_spec, expert_spec)
    return jax.shard_map(device_fn, mesh=mesh, in_specs=in_specs, out_specs=batch_spec, check_vma=False)
```

```python
import functools

import numpy as np
import jax
import jax.numpy as jnp
from jax import lax
from jax.experimental import pallas as pl
from jax.experimental.pallas import tpu as pltpu
from jax.sharding import PartitionSpec as P

NORM_EPS = 1e-6
ROPE_BASE = 10000.0
MESH = pl.DeviceIdType.MESH
LAST_DIMS = (((1,), (1,)), ((), ()))
F32 = jnp.float32
BF16 = jnp.bfloat16

ROWS = 128
HEADS = 8
HD = 128
DIM = 2048
HALF = DIM // 2
HH = HEADS // 2
GROUP = 8
KV_RING = 8
PAIRS = ROWS // (2 * GROUP)
RING = 20
QW = 512
LAYER = 0
S_PART, S_IDS, S_M, S_IN, S_GATES, S_U = range(6)
CORE_ROWS = ROWS // 2
X_LINK, Y_LINK, RELAY = range(3)
XE = 8
EXPERTS = 16
SLOTS = 32
CHUNKS = 4
CW = HALF // CHUNKS
ROWS_Y = (72, 104, 72, 64)


def norm_rows(rows_f, gain):
    inv_rms = lax.rsqrt(jnp.mean(rows_f * rows_f, axis=-1, keepdims=True) + NORM_EPS)
    return (rows_f * inv_rms * gain).astype(BF16)


def attn_kernel(lens_hbm, hidden_ref, gain_hbm, freq_hbm, wq_ref, wkv_ref, kc_ref, vc_ref, ctx_ref,
                lens_ref, gain_ref, freq_ref, small_sem, xbuf, nbuf, cosbuf, sinbuf, wbuf, pos_buf, qbuf, nkbuf, nvbuf, cbuf, sbuf, pbuf, kbuf, vbuf, xsem, wsem, ksem, vsem):
    side = lax.axis_index('side')
    row0 = (side // 2) * ROWS
    core = side % 2
    h0 = core * HEADS

    def size_of(tok):
        return (lens_ref[row0 + tok] + 15) & -16

    def first_token(unit, d):
        return (unit & (PAIRS - 1)) * (2 * GROUP) + d * GROUP

    def start_unit(unit):
        slot = unit & (KV_RING - 1)
        heads = pl.ds(h0 + (unit >> 3) * HH, HH)
        for d in range(2):
            for i in range(GROUP):
                tok = first_token(unit, d) + i
                size = pl.multiple_of(size_of(tok), 16)
                for src, dst, sem in ((kc_ref, kbuf, ksem), (vc_ref, vbuf, vsem)):
                    pltpu.make_async_copy(src.at[LAYER, row0 + tok, heads, pl.ds(0, size), :],
                                          dst.at[slot, pl.ds(d * HH, HH), pl.ds(i * HD, size), :], sem.at[slot, d]).start()

    def wait_unit(unit, buf, sem):
        slot = unit & (KV_RING - 1)
        for d in range(2):
            total = sum(size_of(first_token(unit, d) + i) for i in range(GROUP))
            whole = buf.at[slot, pl.ds(d * HH, HH), pl.ds(0, pl.multiple_of(total, 16)), :]
            pltpu.make_async_copy(whole, whole, sem.at[slot, d]).wait()

    small = [pltpu.make_async_copy(src, dst, small_sem.at[i])
             for i, (src, dst) in enumerate(((lens_hbm, lens_ref), (freq_hbm, freq_ref), (gain_hbm, gain_ref)))]
    for cp in small:
        cp.start()
    x_cp = pltpu.make_async_copy(hidden_ref.at[pl.ds(row0, ROWS), :], xbuf, xsem)
    x_cp.start()

    def weight_copy(j, kind):
        col = core * HALF + j * QW
        if kind == 0:
            src = wq_ref.at[LAYER, :, pl.ds(col, QW)]
        else:
            src = wkv_ref.at[LAYER, :, pl.ds((kind - 1) * DIM + col, QW)]
        return pltpu.make_async_copy(src, wbuf.at[j * 3 + kind], wsem.at[j * 3 + kind])

    def start_units(lo, hi):
        def one(unit, carry):
            for h in range(2 * HH):
                vbuf[unit, h] = jnp.zeros((GROUP * HD, HD), BF16)
            start_unit(unit)
            return carry
        lax.fori_loop(lo, hi, one, 0)
    for kind in range(3):
        weight_copy(0, kind).start()

    for cp in small:
        cp.wait()

    def fill_pos(i, carry):
        for r in range(8):
            row = i * 8 + r
            pos_buf[pl.ds(row, 1), :] = jnp.full((1, HD), lens_ref[row0 + row].astype(F32), F32)
        return carry
    lax.fori_loop(0, ROWS // 8, fill_pos, 0)
    angles = pos_buf[...] * freq_ref[...]
    cosine = jnp.cos(angles)
    lane = lax.broadcasted_iota(jnp.int32, (ROWS, HD), 1)
    sine = jnp.sin(angles)
    sine = jnp.where(lane < HD // 2, -sine, sine)

    start_units(0, 2)
    for kind in range(3):
        weight_copy(1, kind).start()
    x_cp.wait()
    nbuf[...] = norm_rows(xbuf[...].astype(F32), gain_ref[...])
    cosbuf[...] = cosine
    sinbuf[...] = sine
    start_units(2, KV_RING)

    def project(j):
        for kind in range(3):
            weight_copy(j, kind).wait()
            res = jnp.dot(nbuf[...], wbuf[j * 3 + kind], preferred_element_type=F32).astype(BF16).astype(F32)
            for hh in range(HH):
                h = j * HH + hh
                val = res[:, hh * HD:(hh + 1) * HD]
                if kind < 2:
                    val = (val * cosbuf[...] + pltpu.roll(val, HD // 2, 1) * sinbuf[...]).astype(BF16).astype(F32)
                (qbuf, nkbuf, nvbuf)[kind][:, h * HD:(h + 1) * HD] = val
    project(0)

    row_id = lax.broadcasted_iota(jnp.int32, (2 * GROUP, HD), 0) & (GROUP - 1)
    lane_f = lax.broadcasted_iota(jnp.int32, (GROUP, HD), 1).astype(F32)

    def parts_of(unit):
        for d in range(2):
            rows = pl.ds(pl.multiple_of(first_token(unit, d), GROUP), GROUP)
            for hp in range(2):
                head = (unit >> 3) * HH + 2 * hp
                cols = [pl.ds(pl.multiple_of((head + p) * HD, HD), HD) for p in range(2)]
                yield 2 * d + hp, d * HH + 2 * hp, rows, cols

    def score_unit(unit):
        slot = unit & (KV_RING - 1)
        zero = jnp.zeros((GROUP, HD), F32)
        for n, at, rows, cols in parts_of(unit):
            valid = lane_f < pos_buf[rows, :]
            valid = jnp.concatenate([valid, valid], axis=0)
            first = jnp.concatenate([qbuf[rows, cols[0]], zero], axis=0)
            second = jnp.concatenate([zero, qbuf[rows, cols[1]]], axis=0)
            lhs = jnp.concatenate([first, second], axis=1).astype(BF16)
            rhs = jnp.concatenate([kbuf[slot, at], kbuf[slot, at + 1]], axis=1)
            full = lax.dot_general(lhs, rhs, LAST_DIMS, preferred_element_type=F32)
            sc = full[:, 0:HD]
            for i in range(1, GROUP):
                sc = jnp.where(row_id == i, full[:, i * HD:(i + 1) * HD], sc)
            sbuf[unit & 1, n] = jnp.where(valid, sc * (HD ** -0.5), -jnp.inf)

    def soften_unit(unit):
        for n, at, rows, cols in parts_of(unit):
            sc = sbuf[unit & 1, n]
            q_k = [jnp.concatenate([ref[rows, c] for c in cols], axis=0) for ref in (qbuf, nkbuf)]
            self_sc = jnp.sum(q_k[0] * q_k[1], axis=-1, keepdims=True) * (HD ** -0.5)
            peak = jnp.maximum(jnp.max(sc, axis=-1, keepdims=True), self_sc)
            wts = jnp.exp(sc - peak)
            self_w = jnp.exp(self_sc - peak)
            denom = jnp.sum(wts, axis=-1, keepdims=True) + self_w
            prob = wts / denom
            self_p = (self_w / denom).astype(BF16).astype(F32)
            wide = jnp.concatenate([jnp.where(row_id == i, prob, 0.0) for i in range(GROUP)], axis=1).astype(BF16)
            pbuf[unit & 1, n] = wide
            for p in range(2):
                cbuf[rows, cols[p]] = self_p[p * GROUP:(p + 1) * GROUP] * nvbuf[rows, cols[p]]

    def value_unit(unit):
        slot = unit & (KV_RING - 1)
        for n, at, rows, cols in parts_of(unit):
            rhs = jnp.concatenate([vbuf[slot, at], vbuf[slot, at + 1]], axis=1)
            ctx = jnp.dot(pbuf[unit & 1, n], rhs, preferred_element_type=F32)
            for p in range(2):
                cbuf[rows, cols[p]] += ctx[p * GROUP:(p + 1) * GROUP, p * HD:(p + 1) * HD]

    last = 2 * PAIRS - 1
    wait_unit(jnp.int32(0), kbuf, ksem)
    score_unit(jnp.int32(0))
    wait_unit(jnp.int32(1), kbuf, ksem)
    soften_unit(jnp.int32(0))
    score_unit(jnp.int32(1))

    def body(unit, carry):
        wait_unit(unit - 1, vbuf, vsem)
        wait_unit(unit + 1, kbuf, ksem)
        value_unit(unit - 1)
        soften_unit(unit)
        score_unit(unit + 1)

        @pl.when(unit - 1 + KV_RING <= last)
        def _():
            start_unit(unit - 1 + KV_RING)
        return carry
    lax.fori_loop(1, PAIRS - 1, body, 0)
    project(1)
    lax.fori_loop(PAIRS - 1, last, body, 0)
    wait_unit(jnp.int32(last - 1), vbuf, vsem)
    wait_unit(jnp.int32(last), vbuf, vsem)
    value_unit(jnp.int32(last - 1))
    soften_unit(jnp.int32(last))
    value_unit(jnp.int32(last))
    ctx_ref[...] = cbuf[...].astype(BF16)


def attention(hidden, lens, gain, w_q, w_kv, k_cache, v_cache):
    freq = ROPE_BASE ** (-np.arange(HD // 2, dtype=np.float64) * 2.0 / HD)
    freq = np.concatenate([freq, freq])[None, :].astype(np.float32)
    any_spec = pl.BlockSpec(memory_space=pl.ANY)
    vmem_spec = pl.BlockSpec(memory_space=pltpu.VMEM)
    return pl.pallas_call(
        attn_kernel,
        out_shape=jax.ShapeDtypeStruct((ROWS, HALF), BF16),
        in_specs=[any_spec] * 8,
        out_specs=vmem_spec,
        scratch_shapes=[
            pltpu.SMEM(lens.shape, jnp.int32),
            pltpu.VMEM((1, DIM), F32),
            pltpu.VMEM((1, HD), F32),
            pltpu.SemaphoreType.DMA((3,)),
            pltpu.VMEM((ROWS, DIM), BF16),
            pltpu.VMEM((ROWS, DIM), BF16),
            pltpu.VMEM((ROWS, HD), F32),
            pltpu.VMEM((ROWS, HD), F32),
            pltpu.VMEM((6, DIM, QW), BF16),
            pltpu.VMEM((ROWS, HD), F32),
            pltpu.VMEM((ROWS, HALF), F32),
            pltpu.VMEM((ROWS, HALF), F32),
            pltpu.VMEM((ROWS, HALF), F32),
            pltpu.VMEM((ROWS, HALF), F32),
            pltpu.VMEM((2, HEADS // 2, 2 * GROUP, HD), F32),
            pltpu.VMEM((2, HEADS // 2, 2 * GROUP, GROUP * HD), BF16),
            pltpu.VMEM((KV_RING, 2 * HH, GROUP * HD, HD), BF16),
            pltpu.VMEM((KV_RING, 2 * HH, GROUP * HD, HD), BF16),
            pltpu.SemaphoreType.DMA,
            pltpu.SemaphoreType.DMA((6,)),
            pltpu.SemaphoreType.DMA((KV_RING, 2)),
            pltpu.SemaphoreType.DMA((KV_RING, 2)),
        ],
        compiler_params=pltpu.CompilerParams(vmem_limit_bytes=60 * HALF * HALF),
        name='attend',
    )(lens, hidden, gain, jnp.asarray(freq), w_q, w_kv, k_cache, v_cache)


def moe_kernel(gain_hbm, ctx_ref, ids_ref, gates_ref, hidden_ref, wo_ref, sg_ref, su_ref, sd_ref, wg_ref, wu_ref, wd_ref, out_ref,
               gain_ref, ring, ctx_own, part, part_in, xbuf, mrow, mhalf, uall, ish, base, ids_all, gates_all, dmat, cg, xe, inner, ybuf, pbuf,
               recv1, send2, recv2, oall,
               ring_sem, x_sem, misc_s, misc_r, u_s, u_r, uf_s, uf_r, in_s, in_r, p1_s, p1_r, p2_s, p2_r,
               os_s, os_r, ox_s, ox_r, of_s, of_r, out_sem):
    inst = lax.axis_index('inst')
    dy = lax.axis_index('dev')
    side = lax.axis_index('side')
    cx = side // 2
    core = side % 2
    blk0 = dy * 2 + cx
    col0 = core * HALF

    def dev_of(y, x, c):
        return (inst, y, x * 2 + c)
    sibling = dev_of(dy, cx, 1 - core)
    x_nbr = dev_of(dy, 1 - cx, core)
    y_nbr = dev_of(1 - dy, cx, core)

    def rdma(src, dst, s_sem, r_sem, dev):
        return pltpu.make_async_remote_copy(src_ref=src, dst_ref=dst, send_sem=s_sem, recv_sem=r_sem,
                                            device_id=dev, device_id_type=MESH)

    def start_wo(j):
        for q in range(2):
            pltpu.make_async_copy(wo_ref.at[LAYER, pl.ds(col0, HALF), pl.ds((2 * j + q) * QW, QW)],
                                  ring.at[j, pl.ds(q * HALF, HALF), :], ring_sem.at[j]).start()

    def start_gate(e, slot):
        pltpu.make_async_copy(wg_ref.at[LAYER, cx * EXPERTS + e, :, pl.ds(core * QW, QW)], ring.at[slot], ring_sem.at[slot]).start()

    def start_up(e, slot):
        pltpu.make_async_copy(wu_ref.at[LAYER, cx * EXPERTS + e, :, pl.ds(core * QW, QW)], ring.at[slot], ring_sem.at[slot]).start()

    def start_down(m, slot):
        k = m >> 2
        g = m & 3
        for i in range(4):
            pltpu.make_async_copy(wd_ref.at[LAYER, cx * EXPERTS + g * 4 + i, :, pl.ds(col0 + k * CW, CW)],
                                  ring.at[slot, pl.ds((i // 2) * HALF, HALF), pl.ds((i % 2) * CW, CW)],
                                  ring_sem.at[slot]).start()

    def wait_slot(slot):
        pltpu.make_async_copy(wg_ref.at[LAYER, 0, :, pl.ds(0, QW)], ring.at[slot], ring_sem.at[slot]).wait()

    def start_gu_block(b):
        e, up = (b - 5) // 2, (b - 5) % 2
        (start_up if up else start_gate)(e, b % RING)

    ctx_in = pltpu.make_async_copy(ctx_ref, ctx_own, x_sem.at[0])
    ctx_in.start()
    start_wo(0)
    start_wo(1)
    own_rows = pl.ds(pl.multiple_of(core * CORE_ROWS, CORE_ROWS), CORE_ROWS)
    sib_rows = pl.ds(pl.multiple_of((1 - core) * CORE_ROWS, CORE_ROWS), CORE_ROWS)
    x_cp = pltpu.make_async_copy(hidden_ref.at[pl.ds(cx * ROWS + core * CORE_ROWS, CORE_ROWS), :], xbuf, x_sem.at[1])
    x_cp.start()
    gain_cp = pltpu.make_async_copy(gain_hbm, gain_ref, x_sem.at[4])
    gain_cp.start()

    barrier = pltpu.get_barrier_semaphore()
    for dev in (sibling, x_nbr, y_nbr):
        pl.semaphore_signal(barrier, inc=1, device_id=dev, device_id_type=MESH)
    pltpu.make_async_copy(sg_ref.at[LAYER, :, pl.ds(core * QW, QW)], ring.at[2], ring_sem.at[2]).start()
    pltpu.make_async_copy(su_ref.at[LAYER, :, pl.ds(core * QW, QW)], ring.at[3], ring_sem.at[3]).start()
    ids_in = pltpu.make_async_copy(ids_ref, ids_all.at[dy], x_sem.at[2])
    gates_in = pltpu.make_async_copy(gates_ref, gates_all.at[dy], x_sem.at[3])
    ids_in.start()
    gates_in.start()
    pl.semaphore_wait(barrier, 3)

    ctx_in.wait()
    ctx_val = ctx_own[...]
    for j in range(2):
        wait_slot(j)
        for q in range(2):
            n = 2 * j + q
            part[:, n * QW:(n + 1) * QW] = jnp.dot(ctx_val, ring[j, q * HALF:(q + 1) * HALF, :], preferred_element_type=F32)
    part_cp = rdma(part.at[sib_rows, :], part_in, misc_s.at[S_PART], misc_r.at[S_PART], sibling)
    part_cp.start()
    for j in range(2):
        pltpu.make_async_copy(sd_ref.at[LAYER, :, pl.ds(col0 + j * QW, QW)], ring.at[4, pl.ds(j * HALF, HALF), :],
                              ring_sem.at[4]).start()
    for b in range(5, 9):
        start_gu_block(b)
    x_cp.wait()
    gain_cp.wait()
    part_cp.wait_recv()
    mid_rows = (xbuf[...].astype(F32) + (part[own_rows, :] + part_in[...])).astype(BF16)
    mrow[...] = mid_rows
    uall[blk0, own_rows, :] = norm_rows(mid_rows.astype(F32), gain_ref[...])

    blk_x = dy * 2 + 1 - cx
    blk_y = (1 - dy) * 2 + cx
    blk_d = (1 - dy) * 2 + 1 - cx

    def u_part(b, c, h):
        return uall.at[b, pl.ds(c * 64 + h * 32, 32), :]

    def u_copy(b, h, which, dev):
        return rdma(u_part(b, core, h), u_part(b, core, h), u_s.at[which, h], u_r.at[which, h], dev)

    def u_fwd(b, c, which, h):
        return rdma(u_part(b, c, h), u_part(b, c, h), uf_s.at[which, h], uf_r.at[which, h], sibling)
    u_copy(blk0, 0, X_LINK, x_nbr).start()
    u_copy(blk0, 1, Y_LINK, y_nbr).start()
    u_copy(blk0, 1, X_LINK, x_nbr).start()
    u_copy(blk0, 0, Y_LINK, y_nbr).start()
    own_cols = pl.ds(pl.multiple_of(col0, HALF), HALF)
    sib_cols = pl.ds(pl.multiple_of((1 - core) * HALF, HALF), HALF)
    u_sib = [rdma(uall.at[blk0, rows, :], uall.at[blk0, rows, :], misc_s.at[S_U], misc_r.at[S_U], sibling)
             for rows in (own_rows, sib_rows)]
    u_sib[0].start()
    m_cp = rdma(mrow.at[:, sib_cols], mhalf.at[own_rows, :], misc_s.at[S_M], misc_r.at[S_M], sibling)
    m_cp.start()
    mhalf[own_rows, :] = mrow[:, own_cols]
    for b in range(9, 22):
        start_gu_block(b)
    ids_in.wait()
    gates_in.wait()
    ids_cp = rdma(ids_all.at[dy], ids_all.at[dy], misc_s.at[S_IDS], misc_r.at[S_IDS], y_nbr)
    gates_cp = rdma(gates_all.at[dy], gates_all.at[dy], misc_s.at[S_GATES], misc_r.at[S_GATES], y_nbr)
    ids_cp.start()
    gates_cp.start()

    wait_slot(2)
    wait_slot(3)
    u_sib[1].wait_recv()
    u_own = uall[blk0]
    gate = jnp.dot(u_own, ring[2], preferred_element_type=F32)
    up = jnp.dot(u_own, ring[3], preferred_element_type=F32)
    ish[core] = (jax.nn.silu(gate) * up).astype(BF16)
    ish_cp = rdma(ish.at[core], ish.at[core], misc_s.at[S_IN], misc_r.at[S_IN], sibling)
    ish_cp.start()
    start_gu_block(22)
    start_gu_block(23)

    expert_id = dy * 32 + cx * EXPERTS + lax.broadcasted_iota(jnp.int32, (EXPERTS, ROWS), 0)
    before = (lax.broadcasted_iota(jnp.int32, (ROWS, ROWS), 0) < lax.broadcasted_iota(jnp.int32, (ROWS, ROWS), 1))
    before = jnp.where(before, 1.0, 0.0).astype(BF16)
    slot_id = lax.broadcasted_iota(jnp.int32, (SLOTS, ROWS), 0).astype(F32)

    def route_block(yb, xb):
        b = yb * 2 + xb
        hit = jnp.zeros((EXPERTS, ROWS), F32)
        wts = jnp.zeros((EXPERTS, ROWS), F32)
        for j in range(8):
            same = ids_all[yb, j:j + 1, xb * ROWS:(xb + 1) * ROWS] == expert_id
            hit = jnp.where(same, 1.0, hit)
            wts = jnp.where(same, gates_all[yb, j:j + 1, xb * ROWS:(xb + 1) * ROWS], wts)
        place = jnp.dot(hit.astype(BF16), before, preferred_element_type=F32)
        place = jnp.where(hit > 0.5, place, -1.0)
        pieces = []
        for e in range(EXPERTS):
            match = place[e:e + 1, :] == slot_id
            dmat[b, e * SLOTS:(e + 1) * SLOTS, :] = jnp.where(match, 1.0, 0.0).astype(BF16)
            pieces.append(jnp.where(match, wts[e:e + 1, :], 0.0))
        for q in range(4):
            part = jnp.concatenate(pieces[q * 4:(q + 1) * 4], axis=0).T
            high = part.astype(BF16)
            rest = part - high.astype(F32)
            mid = rest.astype(BF16)
            low = (rest - mid.astype(F32)).astype(BF16)
            cg[b, 0:ROWS, q * ROWS:(q + 1) * ROWS] = high
            cg[b, ROWS:256, q * ROWS:(q + 1) * ROWS] = mid
            cg[b, 256:384, q * ROWS:(q + 1) * ROWS] = low

    for xb in range(2):
        route_block(dy, xb)

    half_rows = XE * SLOTS

    def dispatch(b, part):
        def one(n, carry):
            cols = pl.ds(pl.multiple_of(n * QW, QW), QW)
            rows = jnp.dot(dmat[b, part * half_rows:(part + 1) * half_rows, :], uall[b, :, cols],
                           preferred_element_type=F32).astype(BF16)
            for e in range(XE):
                xe[e, pl.ds(pl.multiple_of(b * SLOTS, SLOTS), SLOTS), cols] = rows[e * SLOTS:(e + 1) * SLOTS, :]
            return carry
        lax.fori_loop(0, DIM // QW, one, 0)

    u_copy(blk_x, 0, X_LINK, x_nbr).wait_recv()
    u_copy(blk_x, 0, RELAY, y_nbr).start()
    u_fwd(blk_x, core, X_LINK, 0).start()
    u_copy(blk_y, 1, Y_LINK, y_nbr).wait_recv()
    u_copy(blk_y, 1, RELAY, x_nbr).start()
    u_fwd(blk_y, core, Y_LINK, 1).start()

    rdma(mrow.at[:, sib_cols], mhalf.at[sib_rows, :], misc_s.at[S_M], misc_r.at[S_M], sibling).wait_recv()
    rdma(ish.at[1 - core], ish.at[1 - core], misc_s.at[S_IN], misc_r.at[S_IN], sibling).wait_recv()
    wait_slot(4)
    for j in range(2):
        acc = jnp.dot(ish[0], ring[4, j * HALF:j * HALF + QW, :], preferred_element_type=F32)
        acc = acc + jnp.dot(ish[1], ring[4, j * HALF + QW:(j + 1) * HALF, :], preferred_element_type=F32)
        base[:, j * QW:(j + 1) * QW] = mhalf[:, j * QW:(j + 1) * QW].astype(F32) + acc.astype(BF16).astype(F32)
    start_gu_block(24)
    dispatch(blk0, 0)
    rdma(ids_all.at[1 - dy], ids_all.at[1 - dy], misc_s.at[S_IDS], misc_r.at[S_IDS], y_nbr).wait_recv()
    rdma(gates_all.at[1 - dy], gates_all.at[1 - dy], misc_s.at[S_GATES], misc_r.at[S_GATES], y_nbr).wait_recv()
    u_copy(blk_x, 1, X_LINK, x_nbr).wait_recv()
    u_fwd(blk_x, core, X_LINK, 1).start()
    u_copy(blk_y, 0, Y_LINK, y_nbr).wait_recv()
    u_fwd(blk_y, core, Y_LINK, 0).start()
    for xb in range(2):
        route_block(1 - dy, xb)
    for h in range(2):
        u_fwd(blk_x, 1 - core, X_LINK, h).wait_recv()
    dispatch(blk_x, 0)
    u_copy(blk_d, 0, RELAY, y_nbr).wait_recv()
    u_fwd(blk_d, core, RELAY, 0).start()
    u_copy(blk_d, 1, RELAY, x_nbr).wait_recv()
    u_fwd(blk_d, core, RELAY, 1).start()
    for h in range(2):
        u_fwd(blk_y, 1 - core, Y_LINK, h).wait_recv()
    dispatch(blk_y, 0)
    for h in range(2):
        u_fwd(blk_d, 1 - core, RELAY, h).wait_recv()
    dispatch(blk_d, 0)

    def in_part(e, c):
        return inner.at[e, :, pl.ds(pl.multiple_of(c * QW, QW), QW)]

    def in_copy(e, c):
        return rdma(in_part(e, c), in_part(e, c), in_s.at[e], in_r.at[e], sibling)

    def expert_pair(p, after):
        slots = [lax.rem(5 + 4 * p + i, RING) for i in range(4)]
        for slot in slots:
            wait_slot(slot)
        for i in range(2):
            e = 2 * p + i
            rows = xe[e & (XE - 1)]
            gate = jnp.dot(rows, ring[slots[2 * i]], preferred_element_type=F32)
            up = jnp.dot(rows, ring[slots[2 * i + 1]], preferred_element_type=F32)
            inner[e, :, pl.ds(pl.multiple_of(core * QW, QW), QW)] = (jax.nn.silu(gate) * up).astype(BF16)
        for i in range(2):
            in_copy(2 * p + i, core).start()
        after(p, slots)

    def refill(p, slots):
        @pl.when(p < 3)
        def _():
            for i in range(2):
                start_gate(2 * p + i + 10, slots[2 * i])
                start_up(2 * p + i + 10, slots[2 * i + 1])

        @pl.when((p >= 3) & (p < 7))
        def _():
            for i in range(4):
                start_down(4 * (p - 3) + i, slots[i])

    lax.fori_loop(0, 4, lambda p, c: (expert_pair(p, refill), c)[1], 0)
    lax.fori_loop(0, 4, lambda b, c: (dispatch(b, 1), c)[1], 0)
    lax.fori_loop(4, 8, lambda p, c: (expert_pair(p, refill), c)[1], 0)

    def split(k):
        return pl.ds(0, ROWS_Y[k]), pl.ds(ROWS_Y[k], ROWS - ROWS_Y[k])

    def stage1(k, i):
        top, low = split(k)
        if i == 0:
            return [rdma(pbuf.at[k, blk_d, part, :], recv1.at[k, 0, part, :], p1_s.at[k, 0, a], p1_r.at[k, 0, a], dev)
                    for a, (part, dev) in enumerate(((top, y_nbr), (low, x_nbr)))]
        return [rdma(pbuf.at[k, b, part, :], recv1.at[k, 1, part, :], p1_s.at[k, 1, a], p1_r.at[k, 1, a], dev)
                for a, (b, part, dev) in enumerate(((blk_y, top, y_nbr), (blk_x, low, x_nbr)))]

    def stage2(k):
        return [rdma(send2.at[k, part, :], recv2.at[k, part, :], p2_s.at[k, a], p2_r.at[k, a], dev)
                for a, (part, dev) in enumerate(zip(split(k), (x_nbr, y_nbr)))]

    def run_stage2(k):
        first, second = stage1(k, 0)
        going = stage2(k)
        first.wait_recv()
        n = ROWS_Y[k]
        send2[k, 0:n, :] = pbuf[k, blk_x, 0:n, :] + recv1[k, 0, 0:n, :]
        going[0].start()
        second.wait_recv()
        send2[k, n:ROWS, :] = pbuf[k, blk_y, n:ROWS, :] + recv1[k, 0, n:ROWS, :]
        going[1].start()

    def o_part(x, c, k):
        return oall.at[x, c, k]

    def store_out(x, c, k, which):
        return pltpu.make_async_copy(o_part(x, c, k), out_part(x, c, k), out_sem.at[which, k])

    def out_part(x, c, k):
        return out_ref.at[pl.ds(x * ROWS, ROWS), pl.ds(pl.multiple_of(c * HALF + k * CW, CW), CW)]

    def o_sib(k, c):
        return rdma(o_part(cx, c, k), out_part(cx, c, k), os_s.at[k], os_r.at[k], sibling)

    def o_x(k, x):
        return rdma(o_part(x, core, k), o_part(x, core, k), ox_s.at[k], ox_r.at[k], x_nbr)

    def o_fwd(k, c):
        return rdma(o_part(1 - cx, c, k), out_part(1 - cx, c, k), of_s.at[k], of_r.at[k], sibling)

    def run_final(k):
        for cp in stage1(k, 1):
            cp.wait_recv()
        for cp in stage2(k):
            cp.wait_recv()
        routed = pbuf[k, blk0] + recv1[k, 1] + recv2[k]
        oall[cx, core, k] = (base[:, k * CW:(k + 1) * CW] + routed).astype(BF16)
        o_x(k, cx).start()
        o_sib(k, core).start()
        store_out(cx, core, k, 0).start()

    def run_forward(k):
        o_x(k, 1 - cx).wait_recv()
        o_fwd(k, core).start()
        store_out(1 - cx, core, k, 1).start()

    for k in range(CHUNKS):
        def down_group(g, carry):
            slot = lax.rem(37 + 4 * k + g, RING)
            wait_slot(slot)
            if k == 0:
                for i in range(4):
                    in_copy(g * 4 + i, 1 - core).wait_recv()
            for i in range(4):
                e = g * 4 + i
                w = ring[slot, (i // 2) * HALF:(i // 2 + 1) * HALF, (i % 2) * CW:(i % 2 + 1) * CW]
                res = jnp.dot(inner[e], w, preferred_element_type=F32).astype(BF16)
                for b in range(4):
                    ybuf[b, pl.ds(pl.multiple_of(e * SLOTS, SLOTS), SLOTS), :] = res[b * SLOTS:(b + 1) * SLOTS, :]
            return carry
        lax.fori_loop(0, 4, down_group, 0)

        def combine(b):
            res = jnp.dot(cg[b], ybuf[b], preferred_element_type=F32)
            pbuf[k, b] = res[0:ROWS] + res[ROWS:256] + res[256:384]
        combine(blk_d)
        for cp in stage1(k, 0):
            cp.start()
        combine(blk_y)
        combine(blk_x)
        for cp in stage1(k, 1):
            cp.start()
        combine(blk0)
        if k >= 1:
            run_stage2(k - 1)
    run_final(0)
    run_stage2(CHUNKS - 1)
    for k in range(1, CHUNKS):
        run_final(k)
        run_forward(k - 1)
    run_forward(CHUNKS - 1)
    for k in range(CHUNKS):
        o_sib(k, 1 - core).wait_recv()
    for k in range(CHUNKS):
        o_fwd(k, 1 - core).wait_recv()

    for cp in (part_cp, m_cp, u_sib[0], ids_cp, gates_cp, ish_cp):
        cp.wait_send()
    for h in range(2):
        u_copy(blk0, h, X_LINK, x_nbr).wait_send()
        u_copy(blk0, h, Y_LINK, y_nbr).wait_send()
        u_fwd(blk_x, core, X_LINK, h).wait_send()
        u_fwd(blk_y, core, Y_LINK, h).wait_send()
        u_fwd(blk_d, core, RELAY, h).wait_send()
    u_copy(blk_x, 0, RELAY, y_nbr).wait_send()
    u_copy(blk_y, 1, RELAY, x_nbr).wait_send()
    for e in range(EXPERTS):
        in_copy(e, core).wait_send()
    for k in range(CHUNKS):
        for cp in stage1(k, 0) + stage1(k, 1) + stage2(k):
            cp.wait_send()
        o_sib(k, core).wait_send()
        o_x(k, cx).wait_send()
        o_fwd(k, core).wait_send()
        store_out(cx, core, k, 0).wait()
        store_out(1 - cx, core, k, 1).wait()


def moe(ctx, ids, gates, gain, hidden, w_o, sg, su, sd, wg, wu, wd):
    any_spec = pl.BlockSpec(memory_space=pl.ANY)
    dma = pltpu.SemaphoreType.DMA
    return pl.pallas_call(
        moe_kernel,
        out_shape=jax.ShapeDtypeStruct(hidden.shape, BF16),
        in_specs=[any_spec] * 12,
        out_specs=any_spec,
        scratch_shapes=[
            pltpu.VMEM((1, DIM), F32),
            pltpu.VMEM((RING, DIM, QW), BF16),
            pltpu.VMEM((ROWS, HALF), BF16),
            pltpu.VMEM((ROWS, DIM), F32),
            pltpu.VMEM((CORE_ROWS, DIM), F32),
            pltpu.VMEM((CORE_ROWS, DIM), BF16),
            pltpu.VMEM((CORE_ROWS, DIM), BF16),
            pltpu.VMEM((ROWS, HALF), BF16),
            pltpu.VMEM((4, ROWS, DIM), BF16),
            pltpu.VMEM((2, ROWS, QW), BF16),
            pltpu.VMEM((ROWS, HALF), F32),
            pltpu.VMEM((2, 8, 2 * ROWS), jnp.int32),
            pltpu.VMEM((2, 8, 2 * ROWS), F32),
            pltpu.VMEM((4, EXPERTS * SLOTS, ROWS), BF16),
            pltpu.VMEM((4, 3 * ROWS, EXPERTS * SLOTS), BF16),
            pltpu.VMEM((XE, 4 * SLOTS, DIM), BF16),
            pltpu.VMEM((EXPERTS, 4 * SLOTS, HALF), BF16),
            pltpu.VMEM((4, EXPERTS * SLOTS, CW), BF16),
            pltpu.VMEM((CHUNKS, 4, ROWS, CW), F32),
            pltpu.VMEM((CHUNKS, 2, ROWS, CW), F32),
            pltpu.VMEM((CHUNKS, ROWS, CW), F32),
            pltpu.VMEM((CHUNKS, ROWS, CW), F32),
            pltpu.VMEM((2, 2, CHUNKS, ROWS, CW), BF16),
            dma((RING,)), dma((5,)), dma((6,)), dma((6,)),
            dma((3, 2)), dma((3, 2)), dma((3, 2)), dma((3, 2)),
            dma((EXPERTS,)), dma((EXPERTS,)),
            dma((CHUNKS, 2, 2)), dma((CHUNKS, 2, 2)), dma((CHUNKS, 2)), dma((CHUNKS, 2)),
            dma((CHUNKS,)), dma((CHUNKS,)), dma((CHUNKS,)), dma((CHUNKS,)), dma((CHUNKS,)), dma((CHUNKS,)),
            dma((2, CHUNKS)),
        ],
        compiler_params=pltpu.CompilerParams(vmem_limit_bytes=63 * HALF * HALF, collective_id=0, has_side_effects=True),
        name='experts',
    )(gain, ctx, ids, gates, hidden, w_o, sg, su, sd, wg, wu, wd)


def solution(mesh):
    batch_spec = P(('inst', 'dev'))
    layer_batch = P(None, ('inst', 'dev'))
    expert_spec = P(None, 'dev')

    def device_fn(hidden, k_cache, v_cache, cache_lens, expert_ids, route_gates, attn_gain, ffn_gain, w_q, w_kv, w_o, shared_gate, shared_up, shared_down, w_gate, w_up, w_down):
        ctx = attention(hidden, cache_lens, attn_gain, w_q, w_kv, k_cache, v_cache)
        return moe(ctx, expert_ids[0].T, route_gates[0].T, ffn_gain, hidden, w_o, shared_gate, shared_up, shared_down, w_gate, w_up, w_down)

    in_specs = (batch_spec, layer_batch, layer_batch, batch_spec, layer_batch, layer_batch, P(), P(), P(), P(), P(), P(), P(), P(), expert_spec, expert_spec, expert_spec)
    return jax.shard_map(device_fn, mesh=mesh, in_specs=in_specs, out_specs=batch_spec, check_vma=False)
```
